512 devices in a mesh: grp: 2 (over y), pen: 128 (over x, z), ch: 2 (over core).
Axes of the slice: x: 4, y: 2, z: 32, core: 2. Of those that a mesh axis runs over, the one named last changes fastest.
The devices are a block of a 4x16x32 slice.
Arguments:
- features: bfloat16 [256, 32, 128, 256], P(('grp', 'pen'), 'ch'), parts along dimension 0, may hold values from -6 to 6
- spectral_weights: bfloat16 [1, 2, 16, 32, 32, 1024], P(None, None, None, None, 'ch', 'pen'), may hold values from -0.75 to 0.75
- bypass_weights: float32 [1, 32, 32], P(None, None, 'ch'), may hold values from -0.75 to 0.75
- bypass_bias: float32 [1, 32], P(None, 'ch'), may hold values from -1 to 1
Outputs:
- features_out: float32 [256, 32, 128, 256], P(('grp', 'pen'), 'ch'), parts along dimension 0
The draws below stay inside these ranges and needn't reach their ends.
There are 2 independent parts, one for each index of `grp`. The reference program is written for one: setup_inputs(seed, part) draws one part's arguments, and reference() takes and returns one part's arrays. A program takes and returns all parts, laid end to end along the dimension named above; an argument that names none is the same for every part. Nothing has to cross between parts.
All inputs are finite; a program needn't handle non-finite values.
Results may differ from the reference program's by a relative error of at most 0.0003.
Values may be sent and summed in bfloat16 or wider, within the bound.
No kernel may reach another device: no remote copies, remote signals or barrier semaphores. Data moves between devices by JAX's collectives and lax.ppermute only.
A program may use at most 64 MiB of HBM per device.

```python
import math
import jax
import jax.numpy as jnp
from jax import lax

C = 32
NX = 128
NY = 128
NZ = 256
MX = 16
MY = 32
MZ = 32
LAYERS = 1


def steps_of(key, dims, shards, low, largest):
    factor_of, own = 1.0, jax.random.fold_in(key, 6)
    for axis_at, blocks in shards:
        draws = jnp.exp(jax.random.uniform(jax.random.fold_in(own, axis_at), (blocks,), jnp.float32, low / len(shards), largest / len(shards)))
        factor_of = factor_of * jnp.repeat(draws, dims[axis_at] // blocks).reshape([-1 if axis == axis_at else 1 for axis in range(len(dims))])
    return factor_of


def noise(key, shape, deviation, reach, cuts=(), kind=jnp.bfloat16):
    values = deviation * jax.random.normal(key, shape, jnp.float32)
    if cuts:
        values = values * steps_of(key, shape, cuts, -0.22, 0.18)
    return jnp.clip(values, -reach, reach).astype(kind)


def setup_inputs(seed: int = 0, part: int = 0) -> dict:
    streams_of = jax.random.split(jax.random.key(seed), 5)
    own_keys = jax.random.split(jax.random.fold_in(streams_of[4], part), 5)
    return {
        "features": noise(own_keys[0], (NX, C, NY, NZ), 1.0, 6.0, ((0, 128), (1, 2))),
        "spectral_weights": noise(streams_of[1], (LAYERS, 2, MX, C, C, MY * MZ), (2 * C) ** -0.5, 0.75, ((4, 2), (5, 128))),
        "bypass_weights": noise(streams_of[2], (LAYERS, C, C), (2 * C) ** -0.5, 0.75, ((2, 2),), jnp.float32),
        "bypass_bias": jnp.clip(jax.random.uniform(streams_of[3], (LAYERS, C), jnp.float32, -1.0, 1.0) * steps_of(streams_of[3], (LAYERS, C), ((1, 2),), -0.4, 0.0), -1.0, 1.0),
    }


HIGHEST = lax.Precision.HIGHEST


def kept_freqs(length, kept_count):
    offsets = jnp.arange(kept_count, dtype=jnp.int32)
    return jnp.where(offsets < kept_count // 2, offsets, length - kept_count + offsets)


def tables(length, kept_count):
    phases = (kept_freqs(length, kept_count)[:, None] * jnp.arange(length, dtype=jnp.int32)[None, :]) % length
    angles = phases.astype(jnp.float32) * (2.0 * math.pi / length)
    return jnp.cos(angles), jnp.sin(angles)


def reference(features, spectral_weights, bypass_weights, bypass_bias):
    cos_x, sin_x = tables(NX, MX)
    cos_y, sin_y = tables(NY, MY)
    cos_z, sin_z = tables(NZ, MZ)

    def forward_slab(x_slab):
        real_z = jnp.einsum('cyz,kz->cyk', x_slab, cos_z, precision=HIGHEST) * NZ ** -0.5
        imag_z = -jnp.einsum('cyz,kz->cyk', x_slab, sin_z, precision=HIGHEST) * NZ ** -0.5
        real_y = (jnp.einsum('ay,cyk->cak', cos_y, real_z, precision=HIGHEST)
                  + jnp.einsum('ay,cyk->cak', sin_y, imag_z, precision=HIGHEST)) * NY ** -0.5
        imag_y = (jnp.einsum('ay,cyk->cak', cos_y, imag_z, precision=HIGHEST)
                  - jnp.einsum('ay,cyk->cak', sin_y, real_z, precision=HIGHEST)) * NY ** -0.5
        return real_y, imag_y

    current = features.astype(jnp.float32)
    for layer_idx in range(LAYERS):
        real_y, imag_y = lax.map(forward_slab, current)
        real_x = (jnp.einsum('jx,xcak->jcak', cos_x, real_y, precision=HIGHEST)
                  + jnp.einsum('jx,xcak->jcak', sin_x, imag_y, precision=HIGHEST)) * NX ** -0.5
        imag_x = (jnp.einsum('jx,xcak->jcak', cos_x, imag_y, precision=HIGHEST)
                  - jnp.einsum('jx,xcak->jcak', sin_x, real_y, precision=HIGHEST)) * NX ** -0.5
        weights = spectral_weights[layer_idx].astype(jnp.float32).reshape(2, MX, C, C, MY, MZ)
        real_g = (jnp.einsum('jiak,jioak->joak', real_x, weights[0], precision=HIGHEST)
                  - jnp.einsum('jiak,jioak->joak', imag_x, weights[1], precision=HIGHEST))
        imag_g = (jnp.einsum('jiak,jioak->joak', imag_x, weights[0], precision=HIGHEST)
                  + jnp.einsum('jiak,jioak->joak', real_x, weights[1], precision=HIGHEST))
        real_h = (jnp.einsum('jx,joak->xoak', cos_x, real_g, precision=HIGHEST)
                  - jnp.einsum('jx,joak->xoak', sin_x, imag_g, precision=HIGHEST)) * MX ** -0.5
        imag_h = (jnp.einsum('jx,joak->xoak', cos_x, imag_g, precision=HIGHEST)
                  + jnp.einsum('jx,joak->xoak', sin_x, real_g, precision=HIGHEST)) * MX ** -0.5
        mixing = bypass_weights[layer_idx].astype(jnp.float32)
        offsets = bypass_bias[layer_idx].astype(jnp.float32)

        def inverse_slab(pieces, mixing=mixing, offsets=offsets):
            x_slab, real_b, imag_b = pieces
            real_a = (jnp.einsum('ay,oak->oyk', cos_y, real_b, precision=HIGHEST)
                      - jnp.einsum('ay,oak->oyk', sin_y, imag_b, precision=HIGHEST)) * MY ** -0.5
            imag_a = (jnp.einsum('ay,oak->oyk', cos_y, imag_b, precision=HIGHEST)
                      + jnp.einsum('ay,oak->oyk', sin_y, real_b, precision=HIGHEST)) * MY ** -0.5
            spectral = (jnp.einsum('oyk,kz->oyz', real_a, cos_z, precision=HIGHEST)
                        - jnp.einsum('oyk,kz->oyz', imag_a, sin_z, precision=HIGHEST)) * MZ ** -0.5
            bypass = jnp.einsum('io,iyz->oyz', mixing, x_slab, precision=HIGHEST)
            return x_slab + jax.nn.gelu(bypass + offsets[:, None, None] + spectral, approximate=True)

        current = lax.map(inverse_slab, (current, real_h, imag_h))
    return current
```

```python
import functools

import jax
import jax.numpy as jnp
import ml_dtypes
import numpy as np
from jax import lax
from jax.experimental import pallas as pl
from jax.experimental.pallas import tpu as pltpu
from jax.sharding import PartitionSpec as P

C = 32
NX = 128
NY = 128
NZ = 256
MX = 16
MY = 32
MZ = 32
KB = 4
K8 = 8
LC = 16

F32 = jnp.float32
BF16 = jnp.bfloat16


def tables(length, kept_count):
    offsets = np.arange(kept_count)
    freqs = np.where(offsets < kept_count // 2, offsets, length - kept_count + offsets)
    angles = (freqs[:, None] * np.arange(length)[None, :] % length) * (2.0 * np.pi / length)
    return np.cos(angles), np.sin(angles)


def halves(table):
    table = np.asarray(table, np.float32)
    high = table.astype(ml_dtypes.bfloat16)
    low = (table - high.astype(np.float32)).astype(ml_dtypes.bfloat16)
    return high, low


@functools.cache
def constants():
    cos_x, sin_x = tables(NX, MX)
    cos_y, sin_y = tables(NY, MY)
    cos_z, sin_z = tables(NZ, MZ)
    tz = np.concatenate(halves(np.concatenate([cos_z, -sin_z], 0) * NZ**-0.5), 0)
    wy = np.concatenate([np.concatenate([cos_y, sin_y], 1), np.concatenate([-sin_y, cos_y], 1)], 0)
    wy = np.concatenate(halves(wy * NY**-0.5), 0)
    wx = np.concatenate([np.stack([cos_x, sin_x], 2), np.stack([-sin_x, cos_x], 2)], 0).reshape(2 * MX, 2 * NX)
    wx = np.concatenate(halves(wx * NX**-0.5), 0)
    vx = np.stack([np.concatenate([cos_x, -sin_x], 0).T, np.concatenate([sin_x, cos_x], 0).T], 1)
    high, low = halves(vx.reshape(2 * NX, 2 * MX) * MX**-0.5)
    vx = np.concatenate([high, low, high], 1)
    vy = np.concatenate([np.concatenate([cos_y, sin_y], 1), np.concatenate([-sin_y, cos_y], 1)], 0)
    vy = np.stack(halves(vy * MY**-0.5), 0)
    vz = np.stack(halves(np.concatenate([cos_z, -sin_z], 0) * MZ**-0.5), 0)
    return tz, wy, wx, vx, vy, vz


def split(value):
    high = value.astype(BF16)
    return high, (value - high.astype(F32)).astype(BF16)


def dot(a, b, dims=((1,), (0,))):
    return lax.dot_general(a, b, (dims, ((), ())), preferred_element_type=F32)


STEPS = 4


def forward_kernel(f_ref, tz_ref, wy_ref, o_ref, z_ref):
    step = pl.program_id(0)
    per = LC // STEPS
    for n in range(per):
        rows = dot(tz_ref[...], f_ref[n], ((1,), (1,)))
        rows = rows[: 2 * MZ] + rows[2 * MZ :]
        at = pl.multiple_of((step * per + n) * K8, K8)
        for part in range(2):
            for b in range(KB):
                lo = part * MZ + b * K8
                z_ref[b, pl.ds(at, K8), part * NY : (part + 1) * NY] = rows[lo : lo + K8]

    @pl.when(step == STEPS - 1)
    def _():
        for b in range(KB):
            high, low = split(z_ref[b])
            out = dot(wy_ref[...], high, ((1,), (1,)))
            out = out[: 2 * MY] + out[2 * MY :] + dot(wy_ref[: 2 * MY], low, ((1,), (1,)))
            for part in range(2):
                o_ref[pl.ds(2 * b + part, MY, stride=2 * KB), :] = out[part * MY : (part + 1) * MY]


def forward(field, tz, wy):
    per = LC // STEPS
    return pl.pallas_call(
        forward_kernel,
        grid=(STEPS,),
        in_specs=[
            pl.BlockSpec((per, NY, NZ), lambda s: (s, 0, 0)),
            pl.BlockSpec(tz.shape, lambda s: (0, 0)),
            pl.BlockSpec(wy.shape, lambda s: (0, 0)),
        ],
        out_specs=pl.BlockSpec((2 * MY * KB, LC * K8), lambda s: (0, 0)),
        out_shape=jax.ShapeDtypeStruct((2 * MY * KB, LC * K8), F32),
        scratch_shapes=[pltpu.VMEM((KB, LC * K8, 2 * NY), F32)],
        name="forward",
    )(field, tz, wy)


def x_forward_kernel(s_ref, wx_ref, o_ref):
    high, low = split(s_ref[...])
    out = dot(wx_ref[...], high)
    o_ref[...] = out[: 2 * MX] + out[2 * MX :] + dot(wx_ref[: 2 * MX], low)


def x_forward(sent, wx):
    return pl.pallas_call(
        x_forward_kernel,
        out_shape=jax.ShapeDtypeStruct((2 * MX, LC * K8), F32),
        name="x_forward",
    )(sent, wx)


def mix_kernel(x_ref, w_ref, vx_ref, o_ref):
    lanes = LC * K8
    within = lax.broadcasted_iota(jnp.int32, (MX, lanes), 1) % K8
    real_g = jnp.zeros((MX, lanes), F32)
    imag_g = jnp.zeros((MX, lanes), F32)
    for i in range(C):
        at = within + (i % LC) * K8
        real = jnp.take_along_axis(x_ref[i // LC, :MX], at, axis=1)
        imag = jnp.take_along_axis(x_ref[i // LC, MX:], at, axis=1)
        w_re = w_ref[0, i].astype(F32)
        w_im = w_ref[1, i].astype(F32)
        real_g += w_re * real - w_im * imag
        imag_g += w_re * imag + w_im * real
    high, low = split(jnp.concatenate([real_g, imag_g], 0))
    o_ref[...] = dot(vx_ref[...], jnp.concatenate([high, high, low], 0))


def mix(both, weights, vx):
    return pl.pallas_call(
        mix_kernel,
        out_shape=jax.ShapeDtypeStruct((2 * NX, LC * K8), F32),
        name="mix",
    )(both, weights, vx)


BYPASS_ROWS = 16


def bypass_kernel(w_ref, bias_ref, f_ref, g_ref, o_ref):
    rows = LC * BYPASS_ROWS
    total = bias_ref[...]
    for n, ref in enumerate((f_ref, g_ref)):
        high, low = split(w_ref[:, n * rows : (n + 1) * rows])
        block = ref[...].reshape(rows, NZ)
        total = total + (dot(high, block) + dot(low, block))
    o_ref[...] = total.reshape(LC, BYPASS_ROWS, NZ)


def bypass_of(weights, bias, own, other):
    block = pl.BlockSpec((LC, BYPASS_ROWS, NZ), lambda s: (0, s, 0))
    return pl.pallas_call(
        bypass_kernel,
        grid=(NY // BYPASS_ROWS,),
        in_specs=[
            pl.BlockSpec(weights.shape, lambda s: (0, 0)),
            pl.BlockSpec(bias.shape, lambda s: (0, 0)),
            block,
            block,
        ],
        out_specs=block,
        out_shape=jax.ShapeDtypeStruct((LC, NY, NZ), F32),
        name="bypass",
    )(weights, bias, own, other)


def inverse_kernel(h_ref, vy_ref, vz_ref, b_ref, f_ref, o_ref, a_ref):
    o = pl.program_id(0)

    @pl.when(o == 0)
    def _():
        for b in range(KB):
            parts = [h_ref[pl.ds(2 * b + part, MY, stride=2 * KB), :] for part in range(2)]
            high, low = split(jnp.concatenate(parts, 0).T)
            a_ref[b] = dot(high, vy_ref[0]) + dot(low, vy_ref[0]) + dot(high, vy_ref[1])

    at = pl.multiple_of(o * K8, K8)
    parts = [
        a_ref[b, pl.ds(at, K8), part * NY : (part + 1) * NY] for part in range(2) for b in range(KB)
    ]
    high, low = split(jnp.concatenate(parts, 0).T)
    value = dot(high, vz_ref[0]) + dot(low, vz_ref[0]) + dot(high, vz_ref[1]) + b_ref[0]
    gelu = 0.5 * value * (1.0 + jnp.tanh(np.sqrt(2.0 / np.pi) * (value + 0.044715 * value * value * value)))
    o_ref[0] = f_ref[0].astype(F32) + gelu


def inverse(sent, vy, vz, pre, field):
    block = pl.BlockSpec((1, NY, NZ), lambda s: (s, 0, 0))
    return pl.pallas_call(
        inverse_kernel,
        grid=(LC,),
        in_specs=[
            pl.BlockSpec((2 * MY * KB, LC * K8), lambda s: (0, 0)),
            pl.BlockSpec(vy.shape, lambda s: (0, 0, 0)),
            pl.BlockSpec(vz.shape, lambda s: (0, 0, 0)),
            block,
            block,
        ],
        out_specs=block,
        out_shape=jax.ShapeDtypeStruct((LC, NY, NZ), F32),
        scratch_shapes=[pltpu.VMEM((KB, LC * K8, 2 * NY), F32)],
        name="inverse",
    )(sent, vy, vz, pre, field)


def exchange(value):
    sent = lax.all_to_all(value.reshape(NX, 2, LC * K8), "pen", 0, 0, tiled=True)
    return sent.reshape(2 * NX, LC * K8)


def local(features, spectral_weights, bypass_weights, bypass_bias):
    tz, wy, wx, vx, vy, vz = constants()
    field = features[0]
    other = lax.ppermute(field, "ch", [(0, 1), (1, 0)])

    modes = exchange(forward(field, tz, wy))

    weights = spectral_weights[0].transpose(0, 2, 1, 3, 4).reshape(2, C, MX, LC * K8)

    core = lax.axis_index("ch")
    mixing = bypass_weights[0].reshape(2, LC, LC)
    mixing = jnp.where(core == 0, mixing, mixing[::-1]).reshape(C, LC)
    eye = jnp.eye(BYPASS_ROWS, dtype=F32)
    spread = mixing.T[:, None, :, None] * eye[None, :, None, :]
    spread = spread.reshape(LC * BYPASS_ROWS, C * BYPASS_ROWS)
    offsets = jnp.repeat(bypass_bias[0], BYPASS_ROWS)[:, None]
    pre = bypass_of(spread, offsets, field, other)

    both = lax.all_gather(x_forward(modes, wx), "ch")
    back = exchange(mix(both, weights, vx))
    return inverse(back, vy, vz, pre, field)[None]


def solution(mesh):
    return jax.shard_map(
        local,
        mesh=mesh,
        in_specs=(
            P(("grp", "pen"), "ch", None, None),
            P(None, None, None, None, "ch", "pen"),
            P(None, None, "ch"),
            P(None, "ch"),
        ),
        out_specs=P(("grp", "pen"), "ch", None, None),
        check_vma=False,
    )
```

```python
import functools

import jax
import jax.numpy as jnp
import ml_dtypes
import numpy as np
from jax import lax
from jax.experimental import pallas as pl
from jax.experimental.pallas import tpu as pltpu
from jax.sharding import Mesh, PartitionSpec as P

C = 32
NX = 128
NY = 128
NZ = 256
MX = 16
MY = 32
MZ = 32
KB = 4
K8 = 8
LC = 16
PX, PZ = 4, 32
ORDER = [(place % PX) * PZ + place // PX for place in range(PX * PZ)]

F32 = jnp.float32
BF16 = jnp.bfloat16


def tables(length, kept_count):
    offsets = np.arange(kept_count)
    freqs = np.where(offsets < kept_count // 2, offsets, length - kept_count + offsets)
    angles = (freqs[:, None] * np.arange(length)[None, :] % length) * (2.0 * np.pi / length)
    return np.cos(angles), np.sin(angles)


def halves(table):
    table = np.asarray(table, np.float32)
    high = table.astype(ml_dtypes.bfloat16)
    low = (table - high.astype(np.float32)).astype(ml_dtypes.bfloat16)
    return high, low


@functools.cache
def constants():
    cos_x, sin_x = (table[:, ORDER] for table in tables(NX, MX))
    cos_y, sin_y = tables(NY, MY)
    cos_z, sin_z = tables(NZ, MZ)
    tz = np.concatenate(halves(np.concatenate([cos_z, -sin_z], 0) * NZ**-0.5), 0)
    wy = np.concatenate([np.concatenate([cos_y, sin_y], 1), np.concatenate([-sin_y, cos_y], 1)], 0)
    wy = np.concatenate(halves(wy * NY**-0.5), 0)
    wx = np.concatenate([np.stack([cos_x, sin_x], 2), np.stack([-sin_x, cos_x], 2)], 0).reshape(2 * MX, 2 * NX)
    wx = np.concatenate(halves(wx * NX**-0.5), 0)
    vx = np.stack([np.concatenate([cos_x, -sin_x], 0).T, np.concatenate([sin_x, cos_x], 0).T], 1)
    high, low = halves(vx.reshape(2 * NX, 2 * MX) * MX**-0.5)
    vx = np.concatenate([high, low, high], 1)
    vy = np.concatenate([np.concatenate([cos_y, sin_y], 1), np.concatenate([-sin_y, cos_y], 1)], 0)
    vy = np.stack(halves(vy * MY**-0.5), 0)
    vz = np.stack(halves(np.concatenate([cos_z, -sin_z], 0) * MZ**-0.5), 0)
    return tz, wy, wx, vx, vy, vz


def split(value):
    high = value.astype(BF16)
    return high, (value - high.astype(F32)).astype(BF16)


def rows_of(b, n, part):
    return pl.ds(2 * PX * b + 2 * n + part, 8, stride=2 * PX * KB)


def dot(a, b, dims=((1,), (0,))):
    return lax.dot_general(a, b, (dims, ((), ())), preferred_element_type=F32)


STEPS = 4
VMEM = pl.BlockSpec(memory_space=pltpu.VMEM)
PARAMS = pltpu.CompilerParams(vmem_limit_bytes=16 << 20)


def near(*values):
    return tuple(pltpu.with_memory_space_constraint(v, pltpu.VMEM) for v in values)


def forward_kernel(f_ref, tz_ref, wy_ref, o_ref, z_ref):
    step = pl.program_id(0)
    per = LC // STEPS
    for n in range(per):
        rows = dot(tz_ref[...], f_ref[n], ((1,), (1,)))
        rows = rows[: 2 * MZ] + rows[2 * MZ :]
        at = pl.multiple_of((step * per + n) * K8, K8)
        for part in range(2):
            for b in range(KB):
                lo = part * MZ + b * K8
                z_ref[b, pl.ds(at, K8), part * NY : (part + 1) * NY] = rows[lo : lo + K8]

    @pl.when(step == STEPS - 1)
    def _():
        for b in range(KB):
            high, low = split(z_ref[b])
            out = dot(wy_ref[...], high, ((1,), (1,)))
            out = out[: 2 * MY] + out[2 * MY :] + dot(wy_ref[: 2 * MY], low, ((1,), (1,)))
            for part in range(2):
                for n in range(PX):
                    lo = part * MY + n * 8
                    o_ref[rows_of(b, n, part), :] = out[lo : lo + 8]


def forward(field, tz, wy):
    per = LC // STEPS
    return pl.pallas_call(
        forward_kernel,
        grid=(STEPS,),
        in_specs=[
            pl.BlockSpec((per, NY, NZ), lambda s: (s, 0, 0)),
            pl.BlockSpec(tz.shape, lambda s: (0, 0)),
            pl.BlockSpec(wy.shape, lambda s: (0, 0)),
        ],
        out_specs=VMEM,
        out_shape=pltpu.VMEM((2 * MY * KB, LC * K8), F32),
        scratch_shapes=[pltpu.VMEM((KB, LC * K8, 2 * NY), F32)],
        name="forward",
        compiler_params=PARAMS,
    )(*(pltpu.with_memory_space_constraint(v, pltpu.HBM) for v in (field, jnp.asarray(tz), jnp.asarray(wy))))


def x_forward_kernel(s_ref, wx_ref, o_ref):
    high, low = split(s_ref[...])
    out = dot(wx_ref[...], high)
    o_ref[...] = out[: 2 * MX] + out[2 * MX :] + dot(wx_ref[: 2 * MX], low)


def x_forward(sent, wx):
    return pl.pallas_call(
        x_forward_kernel,
        in_specs=[VMEM] * 2,
        out_specs=VMEM,
        out_shape=pltpu.VMEM((2 * MX, LC * K8), F32),
        name="x_forward",
        compiler_params=PARAMS,
    )(*near(sent, wx))


def mix_kernel(x_ref, w_ref, vx_ref, o_ref):
    lanes = LC * K8
    within = lax.broadcasted_iota(jnp.int32, (MX, lanes), 1) % K8
    real_g = jnp.zeros((MX, lanes), F32)
    imag_g = jnp.zeros((MX, lanes), F32)
    for i in range(C):
        at = within + (i % LC) * K8
        real = jnp.take_along_axis(x_ref[i // LC, :MX], at, axis=1)
        imag = jnp.take_along_axis(x_ref[i // LC, MX:], at, axis=1)
        w_re = w_ref[0, i].astype(F32)
        w_im = w_ref[1, i].astype(F32)
        real_g += w_re * real - w_im * imag
        imag_g += w_re * imag + w_im * real
    high, low = split(jnp.concatenate([real_g, imag_g], 0))
    o_ref[...] = dot(vx_ref[...], jnp.concatenate([high, high, low], 0))


def mix(both, weights, vx):
    return pl.pallas_call(
        mix_kernel,
        in_specs=[VMEM] * 3,
        out_specs=VMEM,
        out_shape=pltpu.VMEM((2 * NX, LC * K8), F32),
        name="mix",
        compiler_params=PARAMS,
    )(*near(both, weights, vx))


BYPASS_ROWS = 16


def bypass_kernel(core_ref, bias_ref, w_ref, f_ref, g_ref, vy_in, vz_in, o_ref, vy_ref, vz_ref, w2_ref):
    rows = LC * BYPASS_ROWS
    step = pl.program_id(0)

    @pl.when(step == 0)
    def _():
        row_of = lax.broadcasted_iota(jnp.int32, (rows, LC), 0) // BYPASS_ROWS
        left = (row_of == lax.broadcasted_iota(jnp.int32, (rows, LC), 1)).astype(BF16)
        same = (
            lax.broadcasted_iota(jnp.int32, (rows, rows), 0) % BYPASS_ROWS
            == lax.broadcasted_iota(jnp.int32, (rows, rows), 1) % BYPASS_ROWS
        )
        col_of = lax.broadcasted_iota(jnp.int32, (C, rows), 1) // BYPASS_ROWS
        channel = lax.broadcasted_iota(jnp.int32, (C, rows), 0)
        core = core_ref[0]
        for n, part in enumerate(split(w_ref[...])):
            tall = dot(left, part).astype(BF16)
            for k in range(2):
                first = LC * (core if k == 0 else 1 - core)
                pick = (channel == col_of + first).astype(BF16)
                w2_ref[k, n] = jnp.where(same, dot(tall, pick), 0.0).astype(BF16)
        vy_ref[...] = vy_in[...]
        vz_ref[...] = vz_in[...]

    at = pl.multiple_of(step * BYPASS_ROWS, BYPASS_ROWS)
    total = None
    for k, ref in enumerate((f_ref, g_ref)):
        block = (ref[:, pl.ds(at, BYPASS_ROWS), :] if k == 0 else ref[...]).reshape(rows, NZ)
        term = dot(w2_ref[k, 0], block) + dot(w2_ref[k, 1], block)
        total = term if total is None else total + term
    for o in range(LC):
        o_ref[o, pl.ds(at, BYPASS_ROWS), :] = total[o * BYPASS_ROWS : (o + 1) * BYPASS_ROWS] + bias_ref[0, o]


def bypass_of(core, bias, weights, own, other, vy, vz):
    rows = LC * BYPASS_ROWS
    smem = pl.BlockSpec(memory_space=pltpu.SMEM)
    whole = pl.BlockSpec(weights.shape, lambda s: (0, 0))
    return pl.pallas_call(
        bypass_kernel,
        grid=(NY // BYPASS_ROWS,),
        in_specs=[smem, smem, whole, VMEM, pl.BlockSpec((LC, BYPASS_ROWS, NZ), lambda s: (0, s, 0))]
        + [pl.BlockSpec(v.shape, lambda s: (0, 0, 0)) for v in (vy, vz)],
        out_specs=[VMEM] * 3,
        out_shape=[pltpu.VMEM((LC, NY, NZ), F32), pltpu.VMEM(vy.shape, BF16), pltpu.VMEM(vz.shape, BF16)],
        scratch_shapes=[pltpu.VMEM((2, 2, rows, rows), BF16)],
        name="bypass",
        compiler_params=PARAMS,
    )(core, bias, weights, *near(own), other, vy, vz)


def stage_kernel(wx_in, vx_in, wx_ref, vx_ref):
    wx_ref[...] = wx_in[...]
    vx_ref[...] = vx_in[...]


def stage(wx, vx):
    return pl.pallas_call(
        stage_kernel,
        out_specs=[VMEM] * 2,
        out_shape=[pltpu.VMEM(wx.shape, BF16), pltpu.VMEM(vx.shape, BF16)],
        name="stage",
        compiler_params=PARAMS,
    )(wx, vx)


INVERSE_STEPS = 4


def inverse_kernel(h_ref, vy_ref, vz_ref, b_ref, f_ref, o_ref, a_ref):
    step = pl.program_id(0)
    per = LC // INVERSE_STEPS

    @pl.when(step == 0)
    def _():
        for b in range(KB):
            parts = [h_ref[rows_of(b, n, part), :] for part in range(2) for n in range(PX)]
            high, low = split(jnp.concatenate(parts, 0).T)
            a_ref[b] = dot(high, vy_ref[0]) + dot(low, vy_ref[0]) + dot(high, vy_ref[1])

    for n in range(per):
        o = step * per + n
        at = pl.multiple_of(o * K8, K8)
        parts = [
            a_ref[b, pl.ds(at, K8), part * NY : (part + 1) * NY] for part in range(2) for b in range(KB)
        ]
        high, low = split(jnp.concatenate(parts, 0).T)
        value = dot(high, vz_ref[0]) + dot(low, vz_ref[0]) + dot(high, vz_ref[1]) + b_ref[o]
        gelu = 0.5 * value * (1.0 + jnp.tanh(np.sqrt(2.0 / np.pi) * (value + 0.044715 * value * value * value)))
        o_ref[n] = f_ref[o].astype(F32) + gelu


def inverse(sent, vy, vz, pre, field):
    return pl.pallas_call(
        inverse_kernel,
        grid=(INVERSE_STEPS,),
        in_specs=[VMEM] * 5,
        out_specs=pl.BlockSpec((LC // INVERSE_STEPS, NY, NZ), lambda s: (s, 0, 0)),
        out_shape=jax.ShapeDtypeStruct((LC, NY, NZ), F32),
        scratch_shapes=[pltpu.VMEM((KB, LC * K8, 2 * NY), F32)],
        name="inverse",
        compiler_params=PARAMS,
    )(*near(sent, vy, vz, pre, field))


def exchange(value):
    sent = lax.all_to_all(value.reshape(NX, 2, LC * K8), ("pz", "px"), 0, 0, tiled=True)
    return sent.reshape(2 * NX, LC * K8)


def local(features, spectral_weights, bypass_weights, bypass_bias):
    tz, wy, wx, vx, vy, vz = constants()
    field = features[0]
    other = lax.ppermute(field, "ch", [(0, 1), (1, 0)])

    modes = exchange(forward(field, tz, wy))

    weights = spectral_weights[0].transpose(0, 2, 1, 3, 4).reshape(2, C, MX, LC * K8)

    core = lax.axis_index("ch").astype(jnp.int32)[None]
    pre, vy, vz = bypass_of(core, bypass_bias, bypass_weights[0].T, field, other, vy, vz)

    wx, vx = stage(wx, vx)
    both = lax.all_gather(x_forward(modes, wx), "ch")
    back = exchange(mix(both, weights, vx))
    return inverse(back, vy, vz, pre, field)[None]


def solution(mesh):
    groups, _, cores = mesh.devices.shape
    chips = Mesh(mesh.devices.reshape(groups, PX, PZ, cores), ("grp", "px", "pz", "ch"))
    return jax.shard_map(
        local,
        mesh=chips,
        in_specs=(
            P(("grp", "px", "pz"), "ch", None, None),
            P(None, None, None, None, "ch", ("px", "pz")),
            P(None, None, "ch"),
            P(None, "ch"),
        ),
        out_specs=P(("grp", "px", "pz"), "ch", None, None),
        check_vma=False,
    )
```

```python
import functools

import jax
import jax.numpy as jnp
import ml_dtypes
import numpy as np
from jax import lax
from jax.experimental import pallas as pl
from jax.experimental.pallas import tpu as pltpu
from jax.sharding import Mesh, PartitionSpec as P

C = 32
NX = 128
NY = 128
NZ = 256
MX = 16
MY = 32
MZ = 32
KB = 4
K8 = 8
LC = 16
PX, PZ = 4, 32
ORDER = [(place % PX) * PZ + place // PX for place in range(PX * PZ)]

F32 = jnp.float32
F16 = jnp.float16
SCALE_MODES = 32.0
SCALE_MIXED = 0.125
BF16 = jnp.bfloat16


def tables(length, kept_count):
    offsets = np.arange(kept_count)
    freqs = np.where(offsets < kept_count // 2, offsets, length - kept_count + offsets)
    angles = (freqs[:, None] * np.arange(length)[None, :] % length) * (2.0 * np.pi / length)
    return np.cos(angles), np.sin(angles)


def halves(table):
    table = np.asarray(table, np.float32)
    high = table.astype(ml_dtypes.bfloat16)
    low = (table - high.astype(np.float32)).astype(ml_dtypes.bfloat16)
    return high, low


@functools.cache
def constants():
    cos_x, sin_x = (table[:, ORDER] for table in tables(NX, MX))
    cos_y, sin_y = tables(NY, MY)
    cos_z, sin_z = tables(NZ, MZ)
    tz = np.concatenate(halves(np.concatenate([cos_z, -sin_z], 0) * NZ**-0.5), 0)
    wy = np.concatenate([np.concatenate([cos_y, sin_y], 1), np.concatenate([-sin_y, cos_y], 1)], 0)
    wy = np.concatenate(halves(wy * (NY**-0.5 * SCALE_MODES)), 0)
    wx = np.concatenate([np.stack([cos_x, sin_x], 2), np.stack([-sin_x, cos_x], 2)], 0).reshape(2 * MX, 2 * NX)
    wx = np.concatenate(halves(wx * (NX**-0.5 / SCALE_MODES)), 0)
    vx = np.stack([np.concatenate([cos_x, -sin_x], 0).T, np.concatenate([sin_x, cos_x], 0).T], 1)
    high, low = halves(vx.reshape(2 * NX, 2 * MX) * (MX**-0.5 * SCALE_MIXED))
    vx = np.concatenate([high, low, high], 1)
    vy = np.concatenate([np.concatenate([cos_y, sin_y], 1), np.concatenate([-sin_y, cos_y], 1)], 0)
    vy = np.stack(halves(vy * (MY**-0.5 / SCALE_MIXED)), 0)
    vz = np.stack(halves(np.concatenate([cos_z, -sin_z], 0) * MZ**-0.5), 0)
    return tz, wy, wx, vx, vy, vz


def split(value):
    high = value.astype(BF16)
    return high, (value - high.astype(F32)).astype(BF16)


def rows_of(b, n, part):
    return pl.ds(2 * PX * b + 2 * n + part, 8, stride=2 * PX * KB)


def dot(a, b, dims=((1,), (0,))):
    return lax.dot_general(a, b, (dims, ((), ())), preferred_element_type=F32)


STEPS = 4
VMEM = pl.BlockSpec(memory_space=pltpu.VMEM)
PARAMS = pltpu.CompilerParams(vmem_limit_bytes=16 << 20)


def near(*values):
    return tuple(pltpu.with_memory_space_constraint(v, pltpu.VMEM) for v in values)


def forward_kernel(f_ref, tz_ref, wy_ref, o_ref, z_ref):
    step = pl.program_id(0)
    per = LC // STEPS
    for n in range(per):
        rows = dot(tz_ref[...], f_ref[n], ((1,), (1,)))
        rows = rows[: 2 * MZ] + rows[2 * MZ :]
        at = pl.multiple_of((step * per + n) * K8, K8)
        for part in range(2):
            for b in range(KB):
                lo = part * MZ + b * K8
                z_ref[b, pl.ds(at, K8), part * NY : (part + 1) * NY] = rows[lo : lo + K8]

    @pl.when(step == STEPS - 1)
    def _():
        for b in range(KB):
            high, low = split(z_ref[b])
            out = dot(wy_ref[...], high, ((1,), (1,)))
            out = out[: 2 * MY] + out[2 * MY :] + dot(wy_ref[: 2 * MY], low, ((1,), (1,)))
            for part in range(2):
                for n in range(PX):
                    lo = part * MY + n * 8
                    o_ref[rows_of(b, n, part), :] = out[lo : lo + 8]


def forward(field, tz, wy):
    per = LC // STEPS
    return pl.pallas_call(
        forward_kernel,
        grid=(STEPS,),
        in_specs=[
            pl.BlockSpec((per, NY, NZ), lambda s: (s, 0, 0)),
            pl.BlockSpec(tz.shape, lambda s: (0, 0)),
            pl.BlockSpec(wy.shape, lambda s: (0, 0)),
        ],
        out_specs=VMEM,
        out_shape=pltpu.VMEM((2 * MY * KB, LC * K8), F32),
        scratch_shapes=[pltpu.VMEM((KB, LC * K8, 2 * NY), F32)],
        name="forward",
        compiler_params=PARAMS,
    )(*(pltpu.with_memory_space_constraint(v, pltpu.HBM) for v in (field, jnp.asarray(tz), jnp.asarray(wy))))


def x_forward_kernel(s_ref, wx_ref, o_ref):
    high, low = split(s_ref[...])
    out = dot(wx_ref[...], high)
    o_ref[...] = out[: 2 * MX] + out[2 * MX :] + dot(wx_ref[: 2 * MX], low)


def x_forward(sent, wx):
    return pl.pallas_call(
        x_forward_kernel,
        in_specs=[VMEM] * 2,
        out_specs=VMEM,
        out_shape=pltpu.VMEM((2 * MX, LC * K8), F32),
        name="x_forward",
        compiler_params=PARAMS,
    )(*near(sent, wx))


def mix_kernel(x_ref, w_ref, vx_ref, o_ref):
    lanes = LC * K8
    within = lax.broadcasted_iota(jnp.int32, (MX, lanes), 1) % K8
    real_g = jnp.zeros((MX, lanes), F32)
    imag_g = jnp.zeros((MX, lanes), F32)
    for i in range(C):
        at = within + (i % LC) * K8
        real = jnp.take_along_axis(x_ref[i // LC, :MX], at, axis=1)
        imag = jnp.take_along_axis(x_ref[i // LC, MX:], at, axis=1)
        w_re = w_ref[0, i].astype(F32)
        w_im = w_ref[1, i].astype(F32)
        real_g += w_re * real - w_im * imag
        imag_g += w_re * imag + w_im * real
    high, low = split(jnp.concatenate([real_g, imag_g], 0))
    o_ref[...] = dot(vx_ref[...], jnp.concatenate([high, high, low], 0))


def mix(both, weights, vx):
    return pl.pallas_call(
        mix_kernel,
        in_specs=[VMEM] * 3,
        out_specs=VMEM,
        out_shape=pltpu.VMEM((2 * NX, LC * K8), F32),
        name="mix",
        compiler_params=PARAMS,
    )(*near(both, weights, vx))


BYPASS_ROWS = 16


def bypass_kernel(core_ref, bias_ref, w_ref, f_ref, g_ref, vy_in, vz_in, o_ref, vy_ref, vz_ref, w2_ref):
    rows = LC * BYPASS_ROWS
    step = pl.program_id(0)

    @pl.when(step == 0)
    def _():
        row_of = lax.broadcasted_iota(jnp.int32, (rows, LC), 0) // BYPASS_ROWS
        left = (row_of == lax.broadcasted_iota(jnp.int32, (rows, LC), 1)).astype(BF16)
        same = (
            lax.broadcasted_iota(jnp.int32, (rows, rows), 0) % BYPASS_ROWS
            == lax.broadcasted_iota(jnp.int32, (rows, rows), 1) % BYPASS_ROWS
        )
        col_of = lax.broadcasted_iota(jnp.int32, (C, rows), 1) // BYPASS_ROWS
        channel = lax.broadcasted_iota(jnp.int32, (C, rows), 0)
        core = core_ref[0]
        for n, part in enumerate(split(w_ref[...])):
            tall = dot(left, part).astype(BF16)
            for k in range(2):
                first = LC * (core if k == 0 else 1 - core)
                pick = (channel == col_of + first).astype(BF16)
                w2_ref[k, n] = jnp.where(same, dot(tall, pick), 0.0).astype(BF16)
        vy_ref[...] = vy_in[...]
        vz_ref[...] = vz_in[...]

    at = pl.multiple_of(step * BYPASS_ROWS, BYPASS_ROWS)
    total = None
    for k, ref in enumerate((f_ref, g_ref)):
        block = (ref[:, pl.ds(at, BYPASS_ROWS), :] if k == 0 else ref[...]).reshape(rows, NZ)
        term = dot(w2_ref[k, 0], block) + dot(w2_ref[k, 1], block)
        total = term if total is None else total + term
    for o in range(LC):
        o_ref[o, pl.ds(at, BYPASS_ROWS), :] = total[o * BYPASS_ROWS : (o + 1) * BYPASS_ROWS] + bias_ref[0, o]


def bypass_of(core, bias, weights, own, other, vy, vz):
    rows = LC * BYPASS_ROWS
    smem = pl.BlockSpec(memory_space=pltpu.SMEM)
    whole = pl.BlockSpec(weights.shape, lambda s: (0, 0))
    return pl.pallas_call(
        bypass_kernel,
        grid=(NY // BYPASS_ROWS,),
        in_specs=[smem, smem, whole, VMEM, pl.BlockSpec((LC, BYPASS_ROWS, NZ), lambda s: (0, s, 0))]
        + [pl.BlockSpec(v.shape, lambda s: (0, 0, 0)) for v in (vy, vz)],
        out_specs=[VMEM] * 3,
        out_shape=[pltpu.VMEM((LC, NY, NZ), F32), pltpu.VMEM(vy.shape, BF16), pltpu.VMEM(vz.shape, BF16)],
        scratch_shapes=[pltpu.VMEM((2, 2, rows, rows), BF16)],
        name="bypass",
        compiler_params=PARAMS,
    )(core, bias, weights, *near(own), other, vy, vz)


def stage_kernel(wx_in, vx_in, wx_ref, vx_ref):
    wx_ref[...] = wx_in[...]
    vx_ref[...] = vx_in[...]


def stage(wx, vx):
    return pl.pallas_call(
        stage_kernel,
        out_specs=[VMEM] * 2,
        out_shape=[pltpu.VMEM(wx.shape, BF16), pltpu.VMEM(vx.shape, BF16)],
        name="stage",
        compiler_params=PARAMS,
    )(wx, vx)


INVERSE_STEPS = 4


def inverse_kernel(h_ref, vy_ref, vz_ref, b_ref, f_ref, o_ref, a_ref):
    step = pl.program_id(0)
    per = LC // INVERSE_STEPS

    @pl.when(step == 0)
    def _():
        for b in range(KB):
            parts = [h_ref[rows_of(b, n, part), :] for part in range(2) for n in range(PX)]
            high, low = split(jnp.concatenate(parts, 0).T)
            a_ref[b] = dot(high, vy_ref[0]) + dot(low, vy_ref[0]) + dot(high, vy_ref[1])

    for n in range(per):
        o = step * per + n
        at = pl.multiple_of(o * K8, K8)
        parts = [
            a_ref[b, pl.ds(at, K8), part * NY : (part + 1) * NY] for part in range(2) for b in range(KB)
        ]
        high, low = split(jnp.concatenate(parts, 0).T)
        value = dot(high, vz_ref[0]) + dot(low, vz_ref[0]) + dot(high, vz_ref[1]) + b_ref[o]
        gelu = 0.5 * value * (1.0 + jnp.tanh(np.sqrt(2.0 / np.pi) * (value + 0.044715 * value * value * value)))
        o_ref[n] = f_ref[o].astype(F32) + gelu


def inverse(sent, vy, vz, pre, field):
    return pl.pallas_call(
        inverse_kernel,
        grid=(INVERSE_STEPS,),
        in_specs=[VMEM] * 5,
        out_specs=pl.BlockSpec((LC // INVERSE_STEPS, NY, NZ), lambda s: (s, 0, 0)),
        out_shape=jax.ShapeDtypeStruct((LC, NY, NZ), F32),
        scratch_shapes=[pltpu.VMEM((KB, LC * K8, 2 * NY), F32)],
        name="inverse",
        compiler_params=PARAMS,
    )(*near(sent, vy, vz, pre, field))


def exchange(value):
    sent = value.astype(F16).reshape(NX, 2, LC * K8)
    sent = lax.all_to_all(sent, ("pz", "px"), 0, 0, tiled=True)
    return sent.reshape(2 * NX, LC * K8).astype(F32)


def local(features, spectral_weights, bypass_weights, bypass_bias):
    tz, wy, wx, vx, vy, vz = constants()
    field = features[0]
    other = lax.ppermute(field, "ch", [(0, 1), (1, 0)])

    modes = exchange(forward(field, tz, wy))

    weights = spectral_weights[0].transpose(0, 2, 1, 3, 4).reshape(2, C, MX, LC * K8)

    core = lax.axis_index("ch").astype(jnp.int32)[None]
    pre, vy, vz = bypass_of(core, bypass_bias, bypass_weights[0].T, field, other, vy, vz)

    wx, vx = stage(wx, vx)
    both = lax.all_gather(x_forward(modes, wx), "ch")
    back = exchange(mix(both, weights, vx))
    return inverse(back, vy, vz, pre, field)[None]


def solution(mesh):
    groups, _, cores = mesh.devices.shape
    chips = Mesh(mesh.devices.reshape(groups, PX, PZ, cores), ("grp", "px", "pz", "ch"))

    return jax.shard_map(
        local,
        mesh=chips,
        in_specs=(
            P(("grp", "px", "pz"), "ch", None, None),
            P(None, None, None, None, "ch", ("px", "pz")),
            P(None, None, "ch"),
            P(None, "ch"),
        ),
        out_specs=P(("grp", "px", "pz"), "ch", None, None),
        check_vma=False,
    )
```

```python
import functools

import jax
import jax.numpy as jnp
import ml_dtypes
import numpy as np
from jax import lax
from jax.experimental import pallas as pl
from jax.experimental.pallas import tpu as pltpu
from jax.sharding import Mesh, PartitionSpec as P

C = 32
NX = 128
NY = 128
NZ = 256
MX = 16
MY = 32
MZ = 32
KB = 4
K8 = 8
LC = 16
PX, PZ = 4, 32
ORDER = [(place % PX) * PZ + place // PX for place in range(PX * PZ)]

F32 = jnp.float32
F16 = jnp.float16
SCALE_MODES = 32.0
SCALE_MIXED = 0.125
BF16 = jnp.bfloat16


def tables(length, kept_count):
    offsets = np.arange(kept_count)
    freqs = np.where(offsets < kept_count // 2, offsets, length - kept_count + offsets)
    angles = (freqs[:, None] * np.arange(length)[None, :] % length) * (2.0 * np.pi / length)
    return np.cos(angles), np.sin(angles)


def halves(table):
    table = np.asarray(table, np.float32)
    high = table.astype(ml_dtypes.bfloat16)
    low = (table - high.astype(np.float32)).astype(ml_dtypes.bfloat16)
    return high, low


@functools.cache
def constants():
    cos_x, sin_x = (table[:, ORDER] for table in tables(NX, MX))
    cos_y, sin_y = tables(NY, MY)
    cos_z, sin_z = tables(NZ, MZ)
    tz = np.concatenate(halves(np.concatenate([cos_z, -sin_z], 0) * NZ**-0.5), 0)
    wy = np.concatenate([np.concatenate([cos_y, sin_y], 1), np.concatenate([-sin_y, cos_y], 1)], 0)
    wy = np.concatenate(halves(wy * (NY**-0.5 * SCALE_MODES)), 0)
    wx = np.concatenate([np.stack([cos_x, sin_x], 2), np.stack([-sin_x, cos_x], 2)], 0).reshape(2 * MX, 2 * NX)
    wx = np.concatenate(halves(wx * (NX**-0.5 / SCALE_MODES)), 0)
    vx = np.stack([np.concatenate([cos_x, -sin_x], 0).T, np.concatenate([sin_x, cos_x], 0).T], 1)
    high, low = halves(vx.reshape(2 * NX, 2 * MX) * (MX**-0.5 * SCALE_MIXED))
    vx = np.concatenate([high, low, high], 1)
    vy = np.concatenate([np.concatenate([cos_y, sin_y], 1), np.concatenate([-sin_y, cos_y], 1)], 0)
    vy = np.stack(halves(vy * (MY**-0.5 / SCALE_MIXED)), 0)
    vz = np.stack(halves(np.concatenate([cos_z, -sin_z], 0) * MZ**-0.5), 0)
    return tz, wy, wx, vx, vy, vz


def split(value):
    high = value.astype(BF16)
    return high, (value - high.astype(F32)).astype(BF16)


def far(*values):
    return tuple(pltpu.with_memory_space_constraint(jnp.asarray(v), pltpu.HBM) for v in values)


def rows_of(b, n, part):
    return pl.ds(2 * PX * b + 2 * n + part, 8, stride=2 * PX * KB)


def dot(a, b, dims=((1,), (0,))):
    return lax.dot_general(a, b, (dims, ((), ())), preferred_element_type=F32)


STEPS = 8
VMEM = pl.BlockSpec(memory_space=pltpu.VMEM)
PARAMS = pltpu.CompilerParams(vmem_limit_bytes=16 << 20)


def near(*values):
    return tuple(pltpu.with_memory_space_constraint(v, pltpu.VMEM) for v in values)


def forward_kernel(f_ref, tz_ref, wy_ref, o_ref, z_ref):
    step = pl.program_id(0)
    per = LC // STEPS
    for n in range(per):
        rows = dot(tz_ref[...], f_ref[n], ((1,), (1,)))
        rows = rows[: 2 * MZ] + rows[2 * MZ :]
        at = pl.multiple_of((step * per + n) * K8, K8)
        for part in range(2):
            for b in range(KB):
                lo = part * MZ + b * K8
                z_ref[b, pl.ds(at, K8), part * NY : (part + 1) * NY] = rows[lo : lo + K8]

    @pl.when(step == STEPS - 1)
    def _():
        for b in range(KB):
            high, low = split(z_ref[b])
            out = dot(wy_ref[...], high, ((1,), (1,)))
            out = out[: 2 * MY] + out[2 * MY :] + dot(wy_ref[: 2 * MY], low, ((1,), (1,)))
            for part in range(2):
                for n in range(PX):
                    lo = part * MY + n * 8
                    o_ref[rows_of(b, n, part), :] = out[lo : lo + 8]


def forward(field, tz, wy):
    per = LC // STEPS
    return pl.pallas_call(
        forward_kernel,
        grid=(STEPS,),
        in_specs=[
            pl.BlockSpec((per, NY, NZ), lambda s: (s, 0, 0)),
            pl.BlockSpec(tz.shape, lambda s: (0, 0)),
            pl.BlockSpec(wy.shape, lambda s: (0, 0)),
        ],
        out_specs=VMEM,
        out_shape=pltpu.VMEM((2 * MY * KB, LC * K8), F32),
        scratch_shapes=[pltpu.VMEM((KB, LC * K8, 2 * NY), F32)],
        name="forward",
        compiler_params=PARAMS,
    )(*far(field, tz, wy))


def x_forward_kernel(s_ref, wx_ref, o_ref):
    high, low = split(s_ref[...])
    out = dot(wx_ref[...], high)
    o_ref[...] = out[: 2 * MX] + out[2 * MX :] + dot(wx_ref[: 2 * MX], low)


def x_forward(sent, wx):
    return pl.pallas_call(
        x_forward_kernel,
        in_specs=[VMEM] * 2,
        out_specs=VMEM,
        out_shape=pltpu.VMEM((2 * MX, LC * K8), F32),
        name="x_forward",
        compiler_params=PARAMS,
    )(*near(sent, wx))


def mix_kernel(x_ref, w_ref, vx_ref, o_ref):
    lanes = LC * K8
    within = lax.broadcasted_iota(jnp.int32, (MX, lanes), 1) % K8
    real_g = jnp.zeros((MX, lanes), F32)
    imag_g = jnp.zeros((MX, lanes), F32)
    for i in range(C):
        at = within + (i % LC) * K8
        real = jnp.take_along_axis(x_ref[i // LC, :MX], at, axis=1)
        imag = jnp.take_along_axis(x_ref[i // LC, MX:], at, axis=1)
        w_re, w_im = w_ref[0, i], w_ref[1, i]
        real_g += w_re * real - w_im * imag
        imag_g += w_re * imag + w_im * real
    high, low = split(jnp.concatenate([real_g, imag_g], 0))
    o_ref[...] = dot(vx_ref[...], jnp.concatenate([high, high, low], 0))


def mix(both, weights, vx):
    return pl.pallas_call(
        mix_kernel,
        in_specs=[VMEM] * 3,
        out_specs=VMEM,
        out_shape=pltpu.VMEM((2 * NX, LC * K8), F32),
        name="mix",
        compiler_params=PARAMS,
    )(*near(both, weights, vx))


BYPASS_ROWS = 16


def bypass_kernel(core_ref, bias_ref, w_ref, f_ref, g_ref, vy_in, vz_in, o_ref, field_ref, vy_ref, vz_ref, w2_ref):
    rows = LC * BYPASS_ROWS
    step = pl.program_id(0)

    @pl.when(step == 0)
    def _():
        row_of = lax.broadcasted_iota(jnp.int32, (rows, LC), 0) // BYPASS_ROWS
        left = (row_of == lax.broadcasted_iota(jnp.int32, (rows, LC), 1)).astype(BF16)
        same = (
            lax.broadcasted_iota(jnp.int32, (rows, rows), 0) % BYPASS_ROWS
            == lax.broadcasted_iota(jnp.int32, (rows, rows), 1) % BYPASS_ROWS
        )
        col_of = lax.broadcasted_iota(jnp.int32, (C, rows), 1) // BYPASS_ROWS
        channel = lax.broadcasted_iota(jnp.int32, (C, rows), 0)
        core = core_ref[0]
        for n, part in enumerate(split(w_ref[...])):
            tall = dot(left, part).astype(BF16)
            for k in range(2):
                first = LC * (core if k == 0 else 1 - core)
                pick = (channel == col_of + first).astype(BF16)
                w2_ref[k, n] = jnp.where(same, dot(tall, pick), 0.0).astype(BF16)
        vy_ref[...] = vy_in[...]
        vz_ref[...] = vz_in[...]

    at = pl.multiple_of(step * BYPASS_ROWS, BYPASS_ROWS)
    total = None
    for k, ref in enumerate((f_ref, g_ref)):
        block = ref[...].reshape(rows, NZ)
        term = dot(w2_ref[k, 0], block) + dot(w2_ref[k, 1], block)
        total = term if total is None else total + term
    field_ref[:, pl.ds(at, BYPASS_ROWS), :] = f_ref[...]
    for o in range(LC):
        o_ref[o, pl.ds(at, BYPASS_ROWS), :] = total[o * BYPASS_ROWS : (o + 1) * BYPASS_ROWS] + bias_ref[0, o]


def bypass_of(core, bias, weights, own, other, vy, vz):
    rows = LC * BYPASS_ROWS
    smem = pl.BlockSpec(memory_space=pltpu.SMEM)
    whole = pl.BlockSpec(weights.shape, lambda s: (0, 0))
    block = pl.BlockSpec((LC, BYPASS_ROWS, NZ), lambda s: (0, s, 0))
    return pl.pallas_call(
        bypass_kernel,
        grid=(NY // BYPASS_ROWS,),
        in_specs=[smem, smem, whole, block, block]
        + [pl.BlockSpec(v.shape, lambda s: (0, 0, 0)) for v in (vy, vz)],
        out_specs=[VMEM] * 4,
        out_shape=[pltpu.VMEM((LC, NY, NZ), F32), pltpu.VMEM((LC, NY, NZ), BF16), pltpu.VMEM(vy.shape, BF16), pltpu.VMEM(vz.shape, BF16)],
        scratch_shapes=[pltpu.VMEM((2, 2, rows, rows), BF16)],
        name="bypass",
        compiler_params=PARAMS,
    )(core, bias, *far(weights, own, other, vy, vz))


def stage_kernel(w_ref, wx_in, vx_in, o_ref, wx_ref, vx_ref):
    wx_ref[...] = wx_in[...]
    vx_ref[...] = vx_in[...]
    for part in range(2):
        for j in range(MX):
            o_ref[part, :, j, :] = w_ref[part, j].astype(F32).T


def stage(weights, wx, vx):
    return pl.pallas_call(
        stage_kernel,
        out_specs=[VMEM] * 3,
        out_shape=[
            pltpu.VMEM((2, C, MX, LC * K8), F32),
            pltpu.VMEM(wx.shape, BF16),
            pltpu.VMEM(vx.shape, BF16),
        ],
        name="stage",
        compiler_params=PARAMS,
    )(*far(weights, wx, vx))


GELU = float(np.sqrt(2.0 / np.pi))
INVERSE_STEPS = 8


def inverse_kernel(h_ref, vy_ref, vz_ref, b_ref, f_ref, o_ref, a_ref):
    step = pl.program_id(0)
    per = LC // INVERSE_STEPS

    @pl.when(step == 0)
    def _():
        for b in range(KB):
            parts = [h_ref[rows_of(b, n, part), :] for part in range(2) for n in range(PX)]
            high, low = split(jnp.concatenate(parts, 0).T)
            a_ref[b] = dot(high, vy_ref[0]) + dot(low, vy_ref[0]) + dot(high, vy_ref[1])

    for n in range(per):
        o = step * per + n
        at = pl.multiple_of(o * K8, K8)
        parts = [
            a_ref[b, pl.ds(at, K8), part * NY : (part + 1) * NY] for part in range(2) for b in range(KB)
        ]
        high, low = split(jnp.concatenate(parts, 0).T)
        value = dot(high, vz_ref[0]) + dot(low, vz_ref[0]) + dot(high, vz_ref[1]) + b_ref[o]
        half = 0.5 * value
        bend = jnp.tanh(value * (GELU + (0.044715 * GELU) * (value * value)))
        o_ref[n] = (f_ref[o].astype(F32) + half) + half * bend


def inverse(sent, vy, vz, pre, field):
    return pl.pallas_call(
        inverse_kernel,
        grid=(INVERSE_STEPS,),
        in_specs=[VMEM] * 5,
        out_specs=pl.BlockSpec((LC // INVERSE_STEPS, NY, NZ), lambda s: (s, 0, 0)),
        out_shape=jax.ShapeDtypeStruct((LC, NY, NZ), F32),
        scratch_shapes=[pltpu.VMEM((KB, LC * K8, 2 * NY), F32)],
        name="inverse",
        compiler_params=PARAMS,
    )(*near(sent, vy, vz, pre, field))


def exchange(value):
    sent = value.astype(F16).reshape(NX, 2, LC * K8)
    sent = lax.all_to_all(sent, ("pz", "px"), 0, 0, tiled=True)
    return sent.reshape(2 * NX, LC * K8).astype(F32)


def local(features, spectral_weights, bypass_weights, bypass_bias):
    tz, wy, wx, vx, vy, vz = constants()
    field = features[0]
    other = lax.ppermute(field, "ch", [(0, 1), (1, 0)])

    modes = exchange(forward(field, tz, wy))

    core = lax.axis_index("ch").astype(jnp.int32)[None]
    pre, near_field, vy, vz = bypass_of(core, bypass_bias, bypass_weights[0].T, field, other, vy, vz)

    weights = spectral_weights[0].transpose(0, 1, 3, 4, 2).reshape(2, MX, LC * K8, C)
    weights, wx, vx = stage(weights, wx, vx)
    both = lax.all_gather(x_forward(modes, wx), "ch")
    back = exchange(mix(both, weights, vx))
    return inverse(back, vy, vz, pre, near_field)[None]


def solution(mesh):
    groups, _, cores = mesh.devices.shape
    chips = Mesh(mesh.devices.reshape(groups, PX, PZ, cores), ("grp", "px", "pz", "ch"))

    return jax.shard_map(
        local,
        mesh=chips,
        in_specs=(
            P(("grp", "px", "pz"), "ch", None, None),
            P(None, None, None, None, "ch", ("px", "pz")),
            P(None, None, "ch"),
            P(None, "ch"),
        ),
        out_specs=P(("grp", "px", "pz"), "ch", None, None),
        check_vma=False,
    )
```

```python
import functools

import jax
import jax.numpy as jnp
import ml_dtypes
import numpy as np
from jax import lax
from jax.experimental import pallas as pl
from jax.experimental.pallas import tpu as pltpu
from jax.sharding import Mesh, PartitionSpec as P

C = 32
NX = 128
NY = 128
NZ = 256
MX = 16
MY = 32
MZ = 32
KB = 4
K8 = 8
LC = 16
PX, PZ = 4, 32
ORDER = [(place % PX) * PZ + place // PX for place in range(PX * PZ)]

F32 = jnp.float32
F16 = jnp.float16
SCALE_MODES = 32.0
SCALE_MIXED = 0.125
BF16 = jnp.bfloat16


def tables(length, kept_count):
    offsets = np.arange(kept_count)
    freqs = np.where(offsets < kept_count // 2, offsets, length - kept_count + offsets)
    angles = (freqs[:, None] * np.arange(length)[None, :] % length) * (2.0 * np.pi / length)
    return np.cos(angles), np.sin(angles)


def halves(table):
    table = np.asarray(table, np.float32)
    high = table.astype(ml_dtypes.bfloat16)
    low = (table - high.astype(np.float32)).astype(ml_dtypes.bfloat16)
    return high, low


@functools.cache
def constants():
    cos_x, sin_x = (table[:, ORDER] for table in tables(NX, MX))
    cos_y, sin_y = tables(NY, MY)
    cos_z, sin_z = tables(NZ, MZ)
    tz = np.concatenate(halves(np.concatenate([cos_z, -sin_z], 0) * NZ**-0.5), 0)
    wy = np.concatenate([np.concatenate([cos_y, sin_y], 1), np.concatenate([-sin_y, cos_y], 1)], 0)
    wy = np.concatenate(halves(wy * (NY**-0.5 * SCALE_MODES)), 0)
    wx = np.concatenate([np.stack([cos_x, sin_x], 2), np.stack([-sin_x, cos_x], 2)], 0).reshape(2 * MX, 2 * NX)
    wx = np.concatenate(halves(wx * (NX**-0.5 / SCALE_MODES)), 0)
    vx = np.stack([np.concatenate([cos_x, -sin_x], 0).T, np.concatenate([sin_x, cos_x], 0).T], 1)
    high, low = halves(vx.reshape(2 * NX, 2 * MX) * (MX**-0.5 * SCALE_MIXED))
    vx = np.concatenate([high, low, high], 1)
    vy = np.concatenate([np.concatenate([cos_y, sin_y], 1), np.concatenate([-sin_y, cos_y], 1)], 0)
    vy = np.stack(halves(vy * (MY**-0.5 / SCALE_MIXED)), 0)
    high, low = halves(np.concatenate([cos_z, -sin_z], 0) * (0.5 * MZ**-0.5))
    vz = np.concatenate([high, high, low], 0)
    return tz, wy, wx, vx, vy, vz


def split(value):
    high = value.astype(BF16)
    return high, (value - high.astype(F32)).astype(BF16)


def far(*values):
    return tuple(pltpu.with_memory_space_constraint(jnp.asarray(v), pltpu.HBM) for v in values)


def rows_of(b, n, part):
    return pl.ds(2 * PX * b + 2 * n + part, 8, stride=2 * PX * KB)


def dot(a, b, dims=((1,), (0,))):
    return lax.dot_general(a, b, (dims, ((), ())), preferred_element_type=F32)


STEPS = 4
VMEM = pl.BlockSpec(memory_space=pltpu.VMEM)
PARAMS = pltpu.CompilerParams(vmem_limit_bytes=16 << 20)


def near(*values):
    return tuple(pltpu.with_memory_space_constraint(v, pltpu.VMEM) for v in values)


def forward_kernel(f_hbm, tz_hbm, wy_hbm, o_ref, f_ref, tz_ref, wy_ref, z_ref, sems):
    per = LC // STEPS
    tz_copy = pltpu.make_async_copy(tz_hbm, tz_ref, sems.at[0])
    wy_copy = pltpu.make_async_copy(wy_hbm, wy_ref, sems.at[1])
    chunks = [
        pltpu.make_async_copy(f_hbm.at[pl.ds(n * per, per)], f_ref.at[pl.ds(n * per, per)], sems.at[2 + n])
        for n in range(STEPS)
    ]
    tz_copy.start()
    for copy in chunks:
        copy.start()
    wy_copy.start()
    tz_copy.wait()
    for n, copy in enumerate(chunks):
        copy.wait()
        for first in range(n * per, (n + 1) * per, 2):
            rows = dot(tz_ref[...], f_ref[first : first + 2].reshape(2 * NY, NZ), ((1,), (1,)))
            rows = rows[: 2 * MZ] + rows[2 * MZ :]
            for i in range(2):
                at = (first + i) * K8
                for part in range(2):
                    for b in range(KB):
                        lo = part * MZ + b * K8
                        z_ref[b, at : at + K8, part * NY : (part + 1) * NY] = rows[lo : lo + K8, i * NY : (i + 1) * NY]
    wy_copy.wait()
    for pair in range(KB // 2):
        high, low = split(z_ref[2 * pair : 2 * pair + 2].reshape(2 * LC * K8, 2 * NY))
        out = dot(wy_ref[...], high, ((1,), (1,)))
        out = out[: 2 * MY] + out[2 * MY :] + dot(wy_ref[: 2 * MY], low, ((1,), (1,)))
        for i in range(2):
            for part in range(2):
                for n in range(PX):
                    lo = part * MY + n * 8
                    o_ref[rows_of(2 * pair + i, n, part), :] = out[lo : lo + 8, i * LC * K8 : (i + 1) * LC * K8]


def forward(field, tz, wy):
    return pl.pallas_call(
        forward_kernel,
        in_specs=[pl.BlockSpec(memory_space=pl.ANY)] * 3,
        out_specs=VMEM,
        out_shape=pltpu.VMEM((2 * MY * KB, LC * K8), F32),
        scratch_shapes=[
            pltpu.VMEM(field.shape, BF16),
            pltpu.VMEM(tz.shape, BF16),
            pltpu.VMEM(wy.shape, BF16),
            pltpu.VMEM((KB, LC * K8, 2 * NY), F32),
            pltpu.SemaphoreType.DMA((2 + STEPS,)),
        ],
        name="forward",
        compiler_params=PARAMS,
    )(*far(field, tz, wy))


def x_forward_kernel(s_ref, wx_ref, o_ref):
    high, low = split(s_ref[...])
    out = dot(wx_ref[...], high)
    o_ref[...] = out[: 2 * MX] + out[2 * MX :] + dot(wx_ref[: 2 * MX], low)


def x_forward(sent, wx):
    return pl.pallas_call(
        x_forward_kernel,
        in_specs=[VMEM] * 2,
        out_specs=VMEM,
        out_shape=pltpu.VMEM((2 * MX, LC * K8), F32),
        name="x_forward",
        compiler_params=PARAMS,
    )(*near(sent, wx))


def mix_kernel(x_ref, w_ref, vx_ref, o_ref):
    lanes = LC * K8
    within = lax.broadcasted_iota(jnp.int32, (MX, lanes), 1) % K8
    real_g = jnp.zeros((MX, lanes), F32)
    imag_g = jnp.zeros((MX, lanes), F32)
    for i in range(C):
        at = within + (i % LC) * K8
        real = jnp.take_along_axis(x_ref[i // LC, :MX], at, axis=1)
        imag = jnp.take_along_axis(x_ref[i // LC, MX:], at, axis=1)
        w_re, w_im = w_ref[0, i], w_ref[1, i]
        real_g += w_re * real - w_im * imag
        imag_g += w_re * imag + w_im * real
    high, low = split(jnp.concatenate([real_g, imag_g], 0))
    o_ref[...] = dot(vx_ref[...], jnp.concatenate([high, high, low], 0))


def mix(both, weights, vx):
    return pl.pallas_call(
        mix_kernel,
        in_specs=[VMEM] * 3,
        out_specs=VMEM,
        out_shape=pltpu.VMEM((2 * NX, LC * K8), F32),
        name="mix",
        compiler_params=PARAMS,
    )(*near(both, weights, vx))


BYPASS_ROWS = 16


def bypass_kernel(core_ref, bias_ref, w_ref, f_ref, g_ref, vy_in, vz_in, o_ref, field_ref, vy_ref, vz_ref, w2_ref):
    rows = LC * BYPASS_ROWS
    step = pl.program_id(0)

    @pl.when(step == 0)
    def _():
        row_of = lax.broadcasted_iota(jnp.int32, (rows, LC), 0) // BYPASS_ROWS
        left = (row_of == lax.broadcasted_iota(jnp.int32, (rows, LC), 1)).astype(BF16)
        same = (
            lax.broadcasted_iota(jnp.int32, (rows, rows), 0) % BYPASS_ROWS
            == lax.broadcasted_iota(jnp.int32, (rows, rows), 1) % BYPASS_ROWS
        )
        col_of = lax.broadcasted_iota(jnp.int32, (C, rows), 1) // BYPASS_ROWS
        channel = lax.broadcasted_iota(jnp.int32, (C, rows), 0)
        core = core_ref[0]
        for n, part in enumerate(split(0.5 * w_ref[...])):
            tall = dot(left, part).astype(BF16)
            for k in range(2):
                first = LC * (core if k == 0 else 1 - core)
                pick = (channel == col_of + first).astype(BF16)
                w2_ref[k, n] = jnp.where(same, dot(tall, pick), 0.0).astype(BF16)
        vy_ref[...] = vy_in[...]
        vz_ref[...] = vz_in[...]

    at = pl.multiple_of(step * BYPASS_ROWS, BYPASS_ROWS)
    total = None
    for k, ref in enumerate((f_ref, g_ref)):
        block = ref[...].reshape(rows, NZ)
        term = dot(w2_ref[k, 0], block) + dot(w2_ref[k, 1], block)
        total = term if total is None else total + term
    field_ref[:, pl.ds(at, BYPASS_ROWS), :] = f_ref[...]
    for o in range(LC):
        o_ref[o, pl.ds(at, BYPASS_ROWS), :] = total[o * BYPASS_ROWS : (o + 1) * BYPASS_ROWS] + 0.5 * bias_ref[0, o]


def bypass_of(core, bias, weights, own, other, vy, vz):
    rows = LC * BYPASS_ROWS
    smem = pl.BlockSpec(memory_space=pltpu.SMEM)
    whole = pl.BlockSpec(weights.shape, lambda s: (0, 0))
    block = pl.BlockSpec((LC, BYPASS_ROWS, NZ), lambda s: (0, s, 0))
    return pl.pallas_call(
        bypass_kernel,
        grid=(NY // BYPASS_ROWS,),
        in_specs=[smem, smem, whole, block, block]
        + [pl.BlockSpec(v.shape, lambda s, n=v.ndim: (0,) * n) for v in (vy, vz)],
        out_specs=[VMEM] * 4,
        out_shape=[pltpu.VMEM((LC, NY, NZ), F32), pltpu.VMEM((LC, NY, NZ), BF16), pltpu.VMEM(vy.shape, BF16), pltpu.VMEM(vz.shape, BF16)],
        scratch_shapes=[pltpu.VMEM((2, 2, rows, rows), BF16)],
        name="bypass",
        compiler_params=PARAMS,
    )(core, bias, *far(weights, own, other, vy, vz))


def stage_kernel(w_ref, wx_in, vx_in, o_ref, wx_ref, vx_ref):
    wx_ref[...] = wx_in[...]
    vx_ref[...] = vx_in[...]
    for part in range(2):
        for j in range(MX):
            o_ref[part, :, j, :] = w_ref[part, j].astype(F32).T


def stage(weights, wx, vx):
    return pl.pallas_call(
        stage_kernel,
        out_specs=[VMEM] * 3,
        out_shape=[
            pltpu.VMEM((2, C, MX, LC * K8), F32),
            pltpu.VMEM(wx.shape, BF16),
            pltpu.VMEM(vx.shape, BF16),
        ],
        name="stage",
        compiler_params=PARAMS,
    )(*far(weights, wx, vx))


GELU = float(np.sqrt(2.0 / np.pi))
TOGETHER = 2


def inverse_kernel(h_ref, vy_ref, vz_ref, b_ref, f_ref, o_hbm, a_ref, out_ref, sems):
    sides = []
    for b in range(KB):
        sides.append(jnp.concatenate([h_ref[rows_of(b, n, part), :] for part in range(2) for n in range(PX)], 0).T)
    high, low = split(jnp.concatenate(sides, 0))
    a_ref[...] = dot(high, vy_ref[0]) + dot(low, vy_ref[0]) + dot(high, vy_ref[1])

    copies = []
    for o in range(LC):
        parts = [
            a_ref[b * LC * K8 + o * K8 : b * LC * K8 + (o + 1) * K8, part * NY : (part + 1) * NY]
            for part in range(2)
            for b in range(KB)
        ]
        high, low = split(jnp.concatenate(parts, 0))
        half = dot(jnp.concatenate([high, low, high], 0).T, vz_ref[...]) + b_ref[o]
        bend = jnp.tanh(half * (2.0 * GELU + (8.0 * 0.044715 * GELU) * (half * half)))
        out_ref[o] = (f_ref[o].astype(F32) + half) + half * bend
        if (o + 1) % TOGETHER == 0:
            rows = pl.ds(o + 1 - TOGETHER, TOGETHER)
            copies.append(pltpu.make_async_copy(out_ref.at[rows], o_hbm.at[rows], sems.at[o // TOGETHER]))
            copies[-1].start()
    for copy in copies:
        copy.wait()


def inverse(sent, vy, vz, pre, field):
    return pl.pallas_call(
        inverse_kernel,
        in_specs=[VMEM] * 5,
        out_specs=pl.BlockSpec(memory_space=pl.ANY),
        out_shape=jax.ShapeDtypeStruct((LC, NY, NZ), F32),
        scratch_shapes=[
            pltpu.VMEM((KB * LC * K8, 2 * NY), F32),
            pltpu.VMEM((LC, NY, NZ), F32),
            pltpu.SemaphoreType.DMA((LC // TOGETHER,)),
        ],
        name="inverse",
        compiler_params=PARAMS,
    )(*near(sent, vy, vz, pre, field))


def exchange(value):
    sent = value.astype(F16).reshape(NX, 2, LC * K8)
    sent = lax.all_to_all(sent, ("pz", "px"), 0, 0, tiled=True)
    return sent.reshape(2 * NX, LC * K8).astype(F32)


def local(features, spectral_weights, bypass_weights, bypass_bias):
    tz, wy, wx, vx, vy, vz = constants()
    field = features[0]
    other = lax.ppermute(field, "ch", [(0, 1), (1, 0)])

    modes = exchange(forward(field, tz, wy))

    core = lax.axis_index("ch").astype(jnp.int32)[None]
    pre, near_field, vy, vz = bypass_of(core, bypass_bias, bypass_weights[0].T, field, other, vy, vz)

    weights = spectral_weights[0].transpose(0, 1, 3, 4, 2).reshape(2, MX, LC * K8, C)
    weights, wx, vx = stage(weights, wx, vx)
    both = lax.all_gather(x_forward(modes, wx), "ch")
    back = exchange(mix(both, weights, vx))
    return inverse(back, vy, vz, pre, near_field)[None]


def solution(mesh):
    groups, _, cores = mesh.devices.shape
    chips = Mesh(mesh.devices.reshape(groups, PX, PZ, cores), ("grp", "px", "pz", "ch"))

    return jax.shard_map(
        local,
        mesh=chips,
        in_specs=(
            P(("grp", "px", "pz"), "ch", None, None),
            P(None, None, None, None, "ch", ("px", "pz")),
            P(None, None, "ch"),
            P(None, "ch"),
        ),
        out_specs=P(("grp", "px", "pz"), "ch", None, None),
        check_vma=False,
    )
```

```python
import functools

import jax
import jax.numpy as jnp
import ml_dtypes
import numpy as np
from jax import lax
from jax.experimental import pallas as pl
from jax.experimental.pallas import tpu as pltpu
from jax.sharding import Mesh, PartitionSpec as P

C = 32
NX = 128
NY = 128
NZ = 256
MX = 16
MY = 32
MZ = 32
KB = 4
K8 = 8
LC = 16
PX, PZ = 4, 32
ORDER = [(place % PX) * PZ + place // PX for place in range(PX * PZ)]

F32 = jnp.float32
F16 = jnp.float16
SCALE_MODES = 32.0
SCALE_MIXED = 0.125
BF16 = jnp.bfloat16


def tables(length, kept_count):
    offsets = np.arange(kept_count)
    freqs = np.where(offsets < kept_count // 2, offsets, length - kept_count + offsets)
    angles = (freqs[:, None] * np.arange(length)[None, :] % length) * (2.0 * np.pi / length)
    return np.cos(angles), np.sin(angles)


def halves(table):
    table = np.asarray(table, np.float32)
    high = table.astype(ml_dtypes.bfloat16)
    low = (table - high.astype(np.float32)).astype(ml_dtypes.bfloat16)
    return high, low


@functools.cache
def constants():
    cos_x, sin_x = (table[:, ORDER] for table in tables(NX, MX))
    cos_y, sin_y = tables(NY, MY)
    cos_z, sin_z = tables(NZ, MZ)
    tz = np.concatenate(halves(np.concatenate([cos_z, -sin_z], 0) * NZ**-0.5), 0)
    wy = np.concatenate([np.concatenate([cos_y, sin_y], 1), np.concatenate([-sin_y, cos_y], 1)], 0)
    wy = np.concatenate(halves(wy * (NY**-0.5 * SCALE_MODES)), 0)
    wx = np.concatenate([np.stack([cos_x, sin_x], 2), np.stack([-sin_x, cos_x], 2)], 0).reshape(2 * MX, 2 * NX)
    wx = np.concatenate(halves(wx * (NX**-0.5 / SCALE_MODES)), 0)
    vx = np.stack([np.concatenate([cos_x, -sin_x], 0).T, np.concatenate([sin_x, cos_x], 0).T], 1)
    high, low = halves(vx.reshape(2 * NX, 2 * MX) * (MX**-0.5 * SCALE_MIXED))
    vx = np.concatenate([high, low, high], 1)
    vy = np.concatenate([np.concatenate([cos_y, sin_y], 1), np.concatenate([-sin_y, cos_y], 1)], 0)
    vy = np.stack(halves(vy * (MY**-0.5 / SCALE_MIXED)), 0)
    high, low = halves(np.concatenate([cos_z, -sin_z], 0) * (0.5 * MZ**-0.5))
    vz = np.concatenate([high, high, low], 0)
    return tz, wy, wx, vx, vy, vz


def split(value):
    high = value.astype(BF16)
    return high, (value - high.astype(F32)).astype(BF16)


def far(*values):
    return tuple(pltpu.with_memory_space_constraint(jnp.asarray(v), pltpu.HBM) for v in values)


def rows_of(b, n, part):
    return pl.ds(2 * PX * b + 2 * n + part, 8, stride=2 * PX * KB)


def dot(a, b, dims=((1,), (0,))):
    return lax.dot_general(a, b, (dims, ((), ())), preferred_element_type=F32)


STEPS = 4
VMEM = pl.BlockSpec(memory_space=pltpu.VMEM)
PARAMS = pltpu.CompilerParams(vmem_limit_bytes=16 << 20)


def near(*values):
    return tuple(pltpu.with_memory_space_constraint(v, pltpu.VMEM) for v in values)


def forward_kernel(f_hbm, tz_hbm, wy_hbm, o_ref, f_ref, tz_ref, wy_ref, z_ref, sems):
    per = LC // STEPS
    tz_copy = pltpu.make_async_copy(tz_hbm, tz_ref, sems.at[0])
    wy_copy = pltpu.make_async_copy(wy_hbm, wy_ref, sems.at[1])
    copies = [pltpu.make_async_copy(f_hbm.at[i], f_ref.at[i], sems.at[2 + i]) for i in range(LC)]
    tz_copy.start()
    for copy in copies:
        copy.start()
    wy_copy.start()
    tz_copy.wait()
    for n in range(STEPS):
        for copy in copies[n * per : (n + 1) * per]:
            copy.wait()
        for first in range(n * per, (n + 1) * per, 2):
            rows = dot(tz_ref[...], f_ref[first : first + 2].reshape(2 * NY, NZ), ((1,), (1,)))
            rows = rows[: 2 * MZ] + rows[2 * MZ :]
            for i in range(2):
                at = (first + i) * K8
                for part in range(2):
                    for b in range(KB):
                        lo = part * MZ + b * K8
                        z_ref[b, at : at + K8, part * NY : (part + 1) * NY] = rows[lo : lo + K8, i * NY : (i + 1) * NY]
    wy_copy.wait()
    for pair in range(KB // 2):
        high, low = split(z_ref[2 * pair : 2 * pair + 2].reshape(2 * LC * K8, 2 * NY))
        out = dot(wy_ref[...], high, ((1,), (1,)))
        out = out[: 2 * MY] + out[2 * MY :] + dot(wy_ref[: 2 * MY], low, ((1,), (1,)))
        for i in range(2):
            for part in range(2):
                for n in range(PX):
                    lo = part * MY + n * 8
                    o_ref[rows_of(2 * pair + i, n, part), :] = out[lo : lo + 8, i * LC * K8 : (i + 1) * LC * K8]


def forward(field, tz, wy):
    return pl.pallas_call(
        forward_kernel,
        in_specs=[pl.BlockSpec(memory_space=pl.ANY)] * 3,
        out_specs=VMEM,
        out_shape=pltpu.VMEM((2 * MY * KB, LC * K8), F32),
        scratch_shapes=[
            pltpu.VMEM(field.shape, BF16),
            pltpu.VMEM(tz.shape, BF16),
            pltpu.VMEM(wy.shape, BF16),
            pltpu.VMEM((KB, LC * K8, 2 * NY), F32),
            pltpu.SemaphoreType.DMA((2 + LC,)),
        ],
        name="forward",
        compiler_params=PARAMS,
    )(*far(field, tz, wy))


def x_forward_kernel(s_ref, wx_ref, o_ref):
    high, low = split(s_ref[...])
    out = dot(wx_ref[...], high)
    o_ref[...] = out[: 2 * MX] + out[2 * MX :] + dot(wx_ref[: 2 * MX], low)


def x_forward(sent, wx):
    return pl.pallas_call(
        x_forward_kernel,
        in_specs=[VMEM] * 2,
        out_specs=VMEM,
        out_shape=pltpu.VMEM((2 * MX, LC * K8), F32),
        name="x_forward",
        compiler_params=PARAMS,
    )(*near(sent, wx))


def mix_kernel(x_ref, w_ref, vx_ref, o_ref):
    lanes = LC * K8
    within = lax.broadcasted_iota(jnp.int32, (MX, lanes), 1) % K8
    real_g = jnp.zeros((MX, lanes), F32)
    imag_g = jnp.zeros((MX, lanes), F32)
    for i in range(C):
        at = within + (i % LC) * K8
        real = jnp.take_along_axis(x_ref[i // LC, :MX], at, axis=1)
        imag = jnp.take_along_axis(x_ref[i // LC, MX:], at, axis=1)
        w_re, w_im = w_ref[0, i], w_ref[1, i]
        real_g += w_re * real - w_im * imag
        imag_g += w_re * imag + w_im * real
    high, low = split(jnp.concatenate([real_g, imag_g], 0))
    o_ref[...] = dot(vx_ref[...], jnp.concatenate([high, high, low], 0))


def mix(both, weights, vx):
    return pl.pallas_call(
        mix_kernel,
        in_specs=[VMEM] * 3,
        out_specs=VMEM,
        out_shape=pltpu.VMEM((2 * NX, LC * K8), F32),
        name="mix",
        compiler_params=PARAMS,
    )(*near(both, weights, vx))


BYPASS_ROWS = 16


def bypass_kernel(core_ref, bias_ref, w_ref, f_ref, g_ref, vy_in, vz_in, o_ref, vy_ref, vz_ref, w2_ref):
    rows = LC * BYPASS_ROWS
    step = pl.program_id(0)

    @pl.when(step == 0)
    def _():
        row_of = lax.broadcasted_iota(jnp.int32, (rows, LC), 0) // BYPASS_ROWS
        left = (row_of == lax.broadcasted_iota(jnp.int32, (rows, LC), 1)).astype(BF16)
        same = (
            lax.broadcasted_iota(jnp.int32, (rows, rows), 0) % BYPASS_ROWS
            == lax.broadcasted_iota(jnp.int32, (rows, rows), 1) % BYPASS_ROWS
        )
        col_of = lax.broadcasted_iota(jnp.int32, (C, rows), 1) // BYPASS_ROWS
        channel = lax.broadcasted_iota(jnp.int32, (C, rows), 0)
        core = core_ref[0]
        for n, part in enumerate(split(0.5 * w_ref[...])):
            tall = dot(left, part).astype(BF16)
            for k in range(2):
                first = LC * (core if k == 0 else 1 - core)
                pick = (channel == col_of + first).astype(BF16)
                w2_ref[k, n] = jnp.where(same, dot(tall, pick), 0.0).astype(BF16)
        vy_ref[...] = vy_in[...]
        vz_ref[...] = vz_in[...]

    at = pl.multiple_of(step * BYPASS_ROWS, BYPASS_ROWS)
    total = None
    for k, ref in enumerate((f_ref, g_ref)):
        block = ref[...].reshape(rows, NZ)
        term = dot(w2_ref[k, 0], block) + dot(w2_ref[k, 1], block)
        total = term if total is None else total + term
    for o in range(LC):
        o_ref[o, pl.ds(at, BYPASS_ROWS), :] = total[o * BYPASS_ROWS : (o + 1) * BYPASS_ROWS] + 0.5 * bias_ref[0, o]


def bypass_of(core, bias, weights, own, other, vy, vz):
    rows = LC * BYPASS_ROWS
    smem = pl.BlockSpec(memory_space=pltpu.SMEM)
    whole = pl.BlockSpec(weights.shape, lambda s: (0, 0))
    block = pl.BlockSpec((LC, BYPASS_ROWS, NZ), lambda s: (0, s, 0))
    return pl.pallas_call(
        bypass_kernel,
        grid=(NY // BYPASS_ROWS,),
        in_specs=[smem, smem, whole, block, block]
        + [pl.BlockSpec(v.shape, lambda s, n=v.ndim: (0,) * n) for v in (vy, vz)],
        out_specs=[VMEM] * 3,
        out_shape=[pltpu.VMEM((LC, NY, NZ), F32), pltpu.VMEM(vy.shape, BF16), pltpu.VMEM(vz.shape, BF16)],
        scratch_shapes=[pltpu.VMEM((2, 2, rows, rows), BF16)],
        name="bypass",
        compiler_params=PARAMS,
    )(core, bias, *far(weights, own, other, vy, vz))


def stage_kernel(w_ref, wx_in, vx_in, o_ref, wx_ref, vx_ref):
    wx_ref[...] = wx_in[...]
    vx_ref[...] = vx_in[...]
    for part in range(2):
        for j in range(MX):
            o_ref[part, :, j, :] = w_ref[part, j].astype(F32).T


def stage(weights, wx, vx):
    return pl.pallas_call(
        stage_kernel,
        out_specs=[VMEM] * 3,
        out_shape=[
            pltpu.VMEM((2, C, MX, LC * K8), F32),
            pltpu.VMEM(wx.shape, BF16),
            pltpu.VMEM(vx.shape, BF16),
        ],
        name="stage",
        compiler_params=PARAMS,
    )(*far(weights, wx, vx))


GELU = float(np.sqrt(2.0 / np.pi))
TOGETHER = 1


def inverse_kernel(h_ref, vy_ref, vz_ref, b_ref, f_hbm, o_hbm, a_ref, f_ref, out_ref, sems, f_sems):
    loads = [pltpu.make_async_copy(f_hbm.at[o], f_ref.at[o], f_sems.at[o]) for o in range(LC)]
    for load in loads:
        load.start()
    sides = []
    for b in range(KB):
        sides.append(jnp.concatenate([h_ref[rows_of(b, n, part), :] for part in range(2) for n in range(PX)], 0).T)
    high, low = split(jnp.concatenate(sides, 0))
    a_ref[...] = dot(high, vy_ref[0]) + dot(low, vy_ref[0]) + dot(high, vy_ref[1])

    copies = []
    for o in range(LC):
        parts = [
            a_ref[b * LC * K8 + o * K8 : b * LC * K8 + (o + 1) * K8, part * NY : (part + 1) * NY]
            for part in range(2)
            for b in range(KB)
        ]
        high, low = split(jnp.concatenate(parts, 0))
        half = dot(jnp.concatenate([high, low, high], 0).T, vz_ref[...]) + b_ref[o]
        bend = jnp.tanh(half * (2.0 * GELU + (8.0 * 0.044715 * GELU) * (half * half)))
        if o in (0, LC // 4):
            for load in loads[o : LC // 4 if o == 0 else LC]:
                load.wait()
        out_ref[o] = (f_ref[o].astype(F32) + half) + half * bend
        if (o + 1) % TOGETHER == 0:
            rows = pl.ds(o + 1 - TOGETHER, TOGETHER)
            copies.append(pltpu.make_async_copy(out_ref.at[rows], o_hbm.at[rows], sems.at[o // TOGETHER]))
            copies[-1].start()
    for copy in copies:
        copy.wait()


def inverse(sent, vy, vz, pre, field):
    return pl.pallas_call(
        inverse_kernel,
        in_specs=[VMEM] * 4 + [pl.BlockSpec(memory_space=pl.ANY)],
        out_specs=pl.BlockSpec(memory_space=pl.ANY),
        out_shape=jax.ShapeDtypeStruct((LC, NY, NZ), F32),
        scratch_shapes=[
            pltpu.VMEM((KB * LC * K8, 2 * NY), F32),
            pltpu.VMEM((LC, NY, NZ), BF16),
            pltpu.VMEM((LC, NY, NZ), F32),
            pltpu.SemaphoreType.DMA((LC // TOGETHER,)),
            pltpu.SemaphoreType.DMA((LC,)),
        ],
        name="inverse",
        compiler_params=PARAMS,
    )(*near(sent, vy, vz, pre), *far(field))


def exchange(value):
    sent = value.astype(F16).reshape(NX, 2, LC * K8)
    sent = lax.all_to_all(sent, ("pz", "px"), 0, 0, tiled=True)
    return sent.reshape(2 * NX, LC * K8).astype(F32)


def local(features, spectral_weights, bypass_weights, bypass_bias):
    tz, wy, wx, vx, vy, vz = constants()
    field = features[0]
    other = lax.ppermute(field, "ch", [(0, 1), (1, 0)])

    modes = exchange(forward(field, tz, wy))

    core = lax.axis_index("ch").astype(jnp.int32)[None]
    pre, vy, vz = bypass_of(core, bypass_bias, bypass_weights[0].T, field, other, vy, vz)

    weights = spectral_weights[0].transpose(0, 1, 3, 4, 2).reshape(2, MX, LC * K8, C)
    weights, wx, vx = stage(weights, wx, vx)
    both = lax.all_gather(x_forward(modes, wx), "ch")
    back = exchange(mix(both, weights, vx))
    return inverse(back, vy, vz, pre, field)[None]


def solution(mesh):
    groups, _, cores = mesh.devices.shape
    chips = Mesh(mesh.devices.reshape(groups, PX, PZ, cores), ("grp", "px", "pz", "ch"))

    return jax.shard_map(
        local,
        mesh=chips,
        in_specs=(
            P(("grp", "px", "pz"), "ch", None, None),
            P(None, None, None, None, "ch", ("px", "pz")),
            P(None, None, "ch"),
            P(None, "ch"),
        ),
        out_specs=P(("grp", "px", "pz"), "ch", None, None),
        check_vma=False,
    )
```

```python
import functools

import jax
import jax.numpy as jnp
import ml_dtypes
import numpy as np
from jax import lax
from jax.experimental import pallas as pl
from jax.experimental.pallas import tpu as pltpu
from jax.sharding import PartitionSpec as P

C = 32
NX = 128
NY = 128
NZ = 256
MX = 16
MY = 32
MZ = 32
KB = 4
K8 = 8
LC = 16
PX, PZ = 4, 32
FIRST_Z = 28
ORDER = [(place % PX) * PZ + (place // PX + FIRST_Z) % PZ for place in range(PX * PZ)]
TURNED = [n * 8 + (m + FIRST_Z // KB) % 8 for n in range(PX) for m in range(8)]

F32 = jnp.float32
F16 = jnp.float16
SCALE_MODES = 32.0
SCALE_MIXED = 0.125
BF16 = jnp.bfloat16


def tables(length, kept_count):
    offsets = np.arange(kept_count)
    freqs = np.where(offsets < kept_count // 2, offsets, length - kept_count + offsets)
    angles = (freqs[:, None] * np.arange(length)[None, :] % length) * (2.0 * np.pi / length)
    return np.cos(angles), np.sin(angles)


def halves(table):
    table = np.asarray(table, np.float32)
    high = table.astype(ml_dtypes.bfloat16)
    low = (table - high.astype(np.float32)).astype(ml_dtypes.bfloat16)
    return high, low


@functools.cache
def constants():
    cos_x, sin_x = (table[:, ORDER] for table in tables(NX, MX))
    cos_y, sin_y = (table[TURNED] for table in tables(NY, MY))
    cos_z, sin_z = tables(NZ, MZ)
    tz = np.concatenate(halves(np.concatenate([cos_z, -sin_z], 0) * NZ**-0.5), 0)
    wy = np.concatenate([np.concatenate([cos_y, sin_y], 1), np.concatenate([-sin_y, cos_y], 1)], 0)
    wy = np.concatenate(halves(wy * (NY**-0.5 * SCALE_MODES)), 0)
    wx = np.concatenate([np.stack([cos_x, sin_x], 2), np.stack([-sin_x, cos_x], 2)], 0).reshape(2 * MX, 2 * NX)
    wx = np.concatenate(halves(wx * (NX**-0.5 / SCALE_MODES)), 0)
    vx = np.stack([np.concatenate([cos_x, -sin_x], 0).T, np.concatenate([sin_x, cos_x], 0).T], 1)
    high, low = halves(vx.reshape(2 * NX, 2 * MX) * (MX**-0.5 * SCALE_MIXED))
    vx = np.concatenate([high, low, high], 1)
    vy = np.concatenate([np.concatenate([cos_y, sin_y], 1), np.concatenate([-sin_y, cos_y], 1)], 0)
    vy = np.stack(halves(vy * (MY**-0.5 / SCALE_MIXED)), 0)
    high, low = halves(np.concatenate([cos_z, -sin_z], 0) * (0.5 * MZ**-0.5))
    vz = np.concatenate([high, high, low], 0)
    return tz, wy, wx, vx, vy, vz


def split(value):
    high = value.astype(BF16)
    return high, (value - high.astype(F32)).astype(BF16)


def far(*values):
    return tuple(pltpu.with_memory_space_constraint(jnp.asarray(v), pltpu.HBM) for v in values)


def rows_of(b, n, part):
    return pl.ds(2 * PX * b + 2 * n + part, 8, stride=2 * PX * KB)


def dot(a, b, dims=((1,), (0,))):
    return lax.dot_general(a, b, (dims, ((), ())), preferred_element_type=F32)


STEPS = 4
VMEM = pl.BlockSpec(memory_space=pltpu.VMEM)
PARAMS = pltpu.CompilerParams(vmem_limit_bytes=16 << 20)


def near(*values):
    return tuple(pltpu.with_memory_space_constraint(v, pltpu.VMEM) for v in values)


def forward_kernel(f_hbm, tz_hbm, wy_hbm, o_ref, f_ref, tz_ref, wy_ref, z_ref, sems):
    per = LC // STEPS
    tz_copy = pltpu.make_async_copy(tz_hbm, tz_ref, sems.at[0])
    wy_copy = pltpu.make_async_copy(wy_hbm, wy_ref, sems.at[1])
    chunks = [
        pltpu.make_async_copy(f_hbm.at[pl.ds(n * per, per)], f_ref.at[pl.ds(n * per, per)], sems.at[2 + n])
        for n in range(STEPS)
    ]
    tz_copy.start()
    for copy in chunks:
        copy.start()
    wy_copy.start()
    tz_copy.wait()
    for n, copy in enumerate(chunks):
        copy.wait()
        for first in range(n * per, (n + 1) * per, 2):
            rows = dot(tz_ref[...], f_ref[first : first + 2].reshape(2 * NY, NZ), ((1,), (1,)))
            rows = rows[: 2 * MZ] + rows[2 * MZ :]
            for i in range(2):
                at = (first + i) * K8
                for part in range(2):
                    for b in range(KB):
                        lo = part * MZ + b * K8
                        z_ref[b, at : at + K8, part * NY : (part + 1) * NY] = rows[lo : lo + K8, i * NY : (i + 1) * NY]
    wy_copy.wait()
    for pair in range(KB // 2):
        high, low = split(z_ref[2 * pair : 2 * pair + 2].reshape(2 * LC * K8, 2 * NY))
        out = dot(wy_ref[...], high, ((1,), (1,)))
        out = out[: 2 * MY] + out[2 * MY :] + dot(wy_ref[: 2 * MY], low, ((1,), (1,)))
        for i in range(2):
            for part in range(2):
                for n in range(PX):
                    lo = part * MY + n * 8
                    o_ref[rows_of(2 * pair + i, n, part), :] = out[lo : lo + 8, i * LC * K8 : (i + 1) * LC * K8]


def forward(field, tz, wy):
    return pl.pallas_call(
        forward_kernel,
        in_specs=[pl.BlockSpec(memory_space=pl.ANY)] * 3,
        out_specs=VMEM,
        out_shape=pltpu.VMEM((2 * MY * KB, LC * K8), F32),
        scratch_shapes=[
            pltpu.VMEM(field.shape, BF16),
            pltpu.VMEM(tz.shape, BF16),
            pltpu.VMEM(wy.shape, BF16),
            pltpu.VMEM((KB, LC * K8, 2 * NY), F32),
            pltpu.SemaphoreType.DMA((2 + STEPS,)),
        ],
        name="forward",
        compiler_params=PARAMS,
    )(*far(field, tz, wy))


def x_forward_kernel(s_ref, wx_ref, o_ref):
    high, low = split(s_ref[...])
    out = dot(wx_ref[...], high)
    o_ref[...] = out[: 2 * MX] + out[2 * MX :] + dot(wx_ref[: 2 * MX], low)


def x_forward(sent, wx):
    return pl.pallas_call(
        x_forward_kernel,
        in_specs=[VMEM] * 2,
        out_specs=VMEM,
        out_shape=pltpu.VMEM((2 * MX, LC * K8), F32),
        name="x_forward",
        compiler_params=PARAMS,
    )(*near(sent, wx))


def mix_kernel(x_ref, w_ref, vx_ref, o_ref):
    lanes = LC * K8
    within = lax.broadcasted_iota(jnp.int32, (MX, lanes), 1) % K8
    real_g = jnp.zeros((MX, lanes), F32)
    imag_g = jnp.zeros((MX, lanes), F32)
    for i in range(C):
        at = within + (i % LC) * K8
        real = jnp.take_along_axis(x_ref[i // LC, :MX], at, axis=1)
        imag = jnp.take_along_axis(x_ref[i // LC, MX:], at, axis=1)
        w_re, w_im = w_ref[0, i], w_ref[1, i]
        real_g += w_re * real - w_im * imag
        imag_g += w_re * imag + w_im * real
    high, low = split(jnp.concatenate([real_g, imag_g], 0))
    o_ref[...] = dot(vx_ref[...], jnp.concatenate([high, high, low], 0))


def mix(both, weights, vx):
    return pl.pallas_call(
        mix_kernel,
        in_specs=[VMEM] * 3,
        out_specs=VMEM,
        out_shape=pltpu.VMEM((2 * NX, LC * K8), F32),
        name="mix",
        compiler_params=PARAMS,
    )(*near(both, weights, vx))


BYPASS_ROWS = 16


def bypass_kernel(core_ref, bias_ref, w_ref, f_ref, g_ref, vy_in, vz_in, o_ref, field_ref, vy_ref, vz_ref, w2_ref):
    rows = LC * BYPASS_ROWS
    step = pl.program_id(0)

    @pl.when(step == 0)
    def _():
        row_of = lax.broadcasted_iota(jnp.int32, (rows, LC), 0) // BYPASS_ROWS
        left = (row_of == lax.broadcasted_iota(jnp.int32, (rows, LC), 1)).astype(BF16)
        same = (
            lax.broadcasted_iota(jnp.int32, (rows, rows), 0) % BYPASS_ROWS
            == lax.broadcasted_iota(jnp.int32, (rows, rows), 1) % BYPASS_ROWS
        )
        col_of = lax.broadcasted_iota(jnp.int32, (C, rows), 1) // BYPASS_ROWS
        channel = lax.broadcasted_iota(jnp.int32, (C, rows), 0)
        core = core_ref[0]
        for n, part in enumerate(split(0.5 * w_ref[...])):
            tall = dot(left, part).astype(BF16)
            for k in range(2):
                first = LC * (core if k == 0 else 1 - core)
                pick = (channel == col_of + first).astype(BF16)
                w2_ref[k, n] = jnp.where(same, dot(tall, pick), 0.0).astype(BF16)
        vy_ref[...] = vy_in[...]
        vz_ref[...] = vz_in[...]

    at = pl.multiple_of(step * BYPASS_ROWS, BYPASS_ROWS)
    total = None
    for k, ref in enumerate((f_ref, g_ref)):
        block = ref[...].reshape(rows, NZ)
        term = dot(w2_ref[k, 0], block) + dot(w2_ref[k, 1], block)
        total = term if total is None else total + term
    field_ref[:, pl.ds(at, BYPASS_ROWS), :] = f_ref[...]
    for o in range(LC):
        o_ref[o, pl.ds(at, BYPASS_ROWS), :] = total[o * BYPASS_ROWS : (o + 1) * BYPASS_ROWS] + 0.5 * bias_ref[0, o]


def bypass_of(core, bias, weights, own, other, vy, vz):
    rows = LC * BYPASS_ROWS
    smem = pl.BlockSpec(memory_space=pltpu.SMEM)
    whole = pl.BlockSpec(weights.shape, lambda s: (0, 0))
    block = pl.BlockSpec((LC, BYPASS_ROWS, NZ), lambda s: (0, s, 0))
    return pl.pallas_call(
        bypass_kernel,
        grid=(NY // BYPASS_ROWS,),
        in_specs=[smem, smem, whole, block, block]
        + [pl.BlockSpec(v.shape, lambda s, n=v.ndim: (0,) * n) for v in (vy, vz)],
        out_specs=[VMEM] * 4,
        out_shape=[pltpu.VMEM((LC, NY, NZ), F32), pltpu.VMEM((LC, NY, NZ), BF16), pltpu.VMEM(vy.shape, BF16), pltpu.VMEM(vz.shape, BF16)],
        scratch_shapes=[pltpu.VMEM((2, 2, rows, rows), BF16)],
        name="bypass",
        compiler_params=PARAMS,
    )(core, bias, *far(weights, own, other, vy, vz))


def stage_kernel(w_ref, wx_in, vx_in, o_ref, wx_ref, vx_ref):
    wx_ref[...] = wx_in[...]
    vx_ref[...] = vx_in[...]
    for part in range(2):
        for j in range(MX):
            o_ref[part, :, j, :] = w_ref[part, j].astype(F32).T


def stage(weights, wx, vx):
    return pl.pallas_call(
        stage_kernel,
        out_specs=[VMEM] * 3,
        out_shape=[
            pltpu.VMEM((2, C, MX, LC * K8), F32),
            pltpu.VMEM(wx.shape, BF16),
            pltpu.VMEM(vx.shape, BF16),
        ],
        name="stage",
        compiler_params=PARAMS,
    )(*far(weights, wx, vx))


GELU = float(np.sqrt(2.0 / np.pi))
TOGETHER = 2


def inverse_kernel(h_ref, vy_ref, vz_ref, b_ref, f_ref, o_hbm, a_ref, out_ref, sems):
    sides = []
    for b in range(KB):
        sides.append(jnp.concatenate([h_ref[rows_of(b, n, part), :] for part in range(2) for n in range(PX)], 0).T)
    high, low = split(jnp.concatenate(sides, 0))
    a_ref[...] = dot(high, vy_ref[0]) + dot(low, vy_ref[0]) + dot(high, vy_ref[1])

    copies = []
    for o in range(LC):
        parts = [
            a_ref[b * LC * K8 + o * K8 : b * LC * K8 + (o + 1) * K8, part * NY : (part + 1) * NY]
            for part in range(2)
            for b in range(KB)
        ]
        high, low = split(jnp.concatenate(parts, 0))
        half = dot(jnp.concatenate([high, low, high], 0).T, vz_ref[...]) + b_ref[o]
        bend = jnp.tanh(half * (2.0 * GELU + (8.0 * 0.044715 * GELU) * (half * half)))
        out_ref[o] = (f_ref[o].astype(F32) + half) + half * bend
        if (o + 1) % TOGETHER == 0:
            rows = pl.ds(o + 1 - TOGETHER, TOGETHER)
            copies.append(pltpu.make_async_copy(out_ref.at[rows], o_hbm.at[rows], sems.at[o // TOGETHER]))
            copies[-1].start()
    for copy in copies:
        copy.wait()


def inverse(sent, vy, vz, pre, field):
    return pl.pallas_call(
        inverse_kernel,
        in_specs=[VMEM] * 5,
        out_specs=pl.BlockSpec(memory_space=pl.ANY),
        out_shape=jax.ShapeDtypeStruct((LC, NY, NZ), F32),
        scratch_shapes=[
            pltpu.VMEM((KB * LC * K8, 2 * NY), F32),
            pltpu.VMEM((LC, NY, NZ), F32),
            pltpu.SemaphoreType.DMA((LC // TOGETHER,)),
        ],
        name="inverse",
        compiler_params=PARAMS,
    )(*near(sent, vy, vz, pre, field))


def exchange(value):
    sent = value.astype(F16).reshape(NX, 2, LC * K8)
    sent = lax.all_to_all(sent, "pen", 0, 0, axis_index_groups=[ORDER], tiled=True)
    return sent.reshape(2 * NX, LC * K8).astype(F32)


def local(features, spectral_weights, bypass_weights, bypass_bias):
    tz, wy, wx, vx, vy, vz = constants()
    field = features[0]
    other = lax.ppermute(field, "ch", [(0, 1), (1, 0)])

    modes = exchange(forward(field, tz, wy))

    core = lax.axis_index("ch").astype(jnp.int32)[None]
    pre, near_field, vy, vz = bypass_of(core, bypass_bias, bypass_weights[0].T, field, other, vy, vz)

    weights = spectral_weights[0].transpose(0, 1, 3, 4, 2).reshape(2, MX, LC * K8, C)
    weights, wx, vx = stage(weights, wx, vx)
    both = lax.all_gather(x_forward(modes, wx), "ch")
    back = exchange(mix(both, weights, vx))
    return inverse(back, vy, vz, pre, near_field)[None]


def solution(mesh):
    return jax.shard_map(
        local,
        mesh=mesh,
        in_specs=(
            P(("grp", "pen"), "ch", None, None),
            P(None, None, None, None, "ch", "pen"),
            P(None, None, "ch"),
            P(None, "ch"),
        ),
        out_specs=P(("grp", "pen"), "ch", None, None),
        check_vma=False,
    )
```

```python
import functools

import jax
import jax.numpy as jnp
import ml_dtypes
import numpy as np
from jax import lax
from jax.experimental import pallas as pl
from jax.experimental.pallas import tpu as pltpu
from jax.sharding import PartitionSpec as P

C = 32
NX = 128
NY = 128
NZ = 256
MX = 16
MY = 32
MZ = 32
KB = 4
K8 = 8
LC = 16
PX, PZ = 4, 32
FIRST_Z = 24
FIRST_X = 2
ORDER = [(place + FIRST_X) % PX * PZ + (place // PX + FIRST_Z) % PZ for place in range(PX * PZ)]
TURNED = [(n + FIRST_X) % PX * 8 + (m + FIRST_Z // KB) % 8 for n in range(PX) for m in range(8)]

F32 = jnp.float32
F16 = jnp.float16
SCALE_MODES = 32.0
SCALE_MIXED = 0.125
BF16 = jnp.bfloat16


def tables(length, kept_count):
    offsets = np.arange(kept_count)
    freqs = np.where(offsets < kept_count // 2, offsets, length - kept_count + offsets)
    angles = (freqs[:, None] * np.arange(length)[None, :] % length) * (2.0 * np.pi / length)
    return np.cos(angles), np.sin(angles)


def halves(table):
    table = np.asarray(table, np.float32)
    high = table.astype(ml_dtypes.bfloat16)
    low = (table - high.astype(np.float32)).astype(ml_dtypes.bfloat16)
    return high, low


@functools.cache
def constants():
    cos_x, sin_x = (table[:, ORDER] for table in tables(NX, MX))
    cos_y, sin_y = (table[TURNED] for table in tables(NY, MY))
    cos_z, sin_z = tables(NZ, MZ)
    tz = np.concatenate(halves(np.concatenate([cos_z, -sin_z], 0) * NZ**-0.5), 0)
    wy = np.concatenate([np.concatenate([cos_y, sin_y], 1), np.concatenate([-sin_y, cos_y], 1)], 0)
    wy = np.concatenate(halves(wy * (NY**-0.5 * SCALE_MODES)), 0)
    wx = np.concatenate([np.stack([cos_x, sin_x], 2), np.stack([-sin_x, cos_x], 2)], 0).reshape(2 * MX, 2 * NX)
    wx = np.concatenate(halves(wx * (NX**-0.5 / SCALE_MODES)), 0)
    vx = np.stack([np.concatenate([cos_x, -sin_x], 0).T, np.concatenate([sin_x, cos_x], 0).T], 1)
    high, low = halves(vx.reshape(2 * NX, 2 * MX) * (MX**-0.5 * SCALE_MIXED))
    vx = np.concatenate([high, low, high], 1)
    vy = np.concatenate([np.concatenate([cos_y, sin_y], 1), np.concatenate([-sin_y, cos_y], 1)], 0)
    vy = np.stack(halves(vy * (MY**-0.5 / SCALE_MIXED)), 0)
    high, low = halves(np.concatenate([cos_z, -sin_z], 0) * (0.5 * MZ**-0.5))
    vz = np.concatenate([high, high, low], 0)
    return tz, wy, wx, vx, vy, vz


def split(value):
    high = value.astype(BF16)
    return high, (value - high.astype(F32)).astype(BF16)


def far(*values):
    return tuple(pltpu.with_memory_space_constraint(jnp.asarray(v), pltpu.HBM) for v in values)


def rows_of(b, n, part):
    return pl.ds(2 * PX * b + 2 * n + part, 8, stride=2 * PX * KB)


def dot(a, b, dims=((1,), (0,))):
    return lax.dot_general(a, b, (dims, ((), ())), preferred_element_type=F32)


STEPS = 2
VMEM = pl.BlockSpec(memory_space=pltpu.VMEM)
PARAMS = pltpu.CompilerParams(vmem_limit_bytes=16 << 20)


def near(*values):
    return tuple(pltpu.with_memory_space_constraint(v, pltpu.VMEM) for v in values)


def forward_kernel(f_hbm, tz_hbm, wy_hbm, o_ref, f_ref, tz_ref, wy_ref, z_ref, sems):
    per = LC // STEPS
    tz_copy = pltpu.make_async_copy(tz_hbm, tz_ref, sems.at[0])
    wy_copy = pltpu.make_async_copy(wy_hbm, wy_ref, sems.at[1])
    chunks = [
        pltpu.make_async_copy(f_hbm.at[pl.ds(n * per, per)], f_ref.at[pl.ds(n * per, per)], sems.at[2 + n])
        for n in range(STEPS)
    ]
    tz_copy.start()
    for copy in chunks:
        copy.start()
    wy_copy.start()
    tz_copy.wait()
    for n, copy in enumerate(chunks):
        copy.wait()
        for first in range(n * per, (n + 1) * per, 2):
            rows = dot(tz_ref[...], f_ref[first : first + 2].reshape(2 * NY, NZ), ((1,), (1,)))
            rows = rows[: 2 * MZ] + rows[2 * MZ :]
            for i in range(2):
                at = (first + i) * K8
                for part in range(2):
                    for b in range(KB):
                        lo = part * MZ + b * K8
                        z_ref[b, at : at + K8, part * NY : (part + 1) * NY] = rows[lo : lo + K8, i * NY : (i + 1) * NY]
    wy_copy.wait()
    for pair in range(KB // 2):
        high, low = split(z_ref[2 * pair : 2 * pair + 2].reshape(2 * LC * K8, 2 * NY))
        out = dot(wy_ref[...], high, ((1,), (1,)))
        out = out[: 2 * MY] + out[2 * MY :] + dot(wy_ref[: 2 * MY], low, ((1,), (1,)))
        for i in range(2):
            for part in range(2):
                for n in range(PX):
                    lo = part * MY + n * 8
                    o_ref[rows_of(2 * pair + i, n, part), :] = out[lo : lo + 8, i * LC * K8 : (i + 1) * LC * K8]


def forward(field, tz, wy):
    return pl.pallas_call(
        forward_kernel,
        in_specs=[pl.BlockSpec(memory_space=pl.ANY)] * 3,
        out_specs=VMEM,
        out_shape=pltpu.VMEM((2 * MY * KB, LC * K8), F32),
        scratch_shapes=[
            pltpu.VMEM(field.shape, BF16),
            pltpu.VMEM(tz.shape, BF16),
            pltpu.VMEM(wy.shape, BF16),
            pltpu.VMEM((KB, LC * K8, 2 * NY), F32),
            pltpu.SemaphoreType.DMA((2 + STEPS,)),
        ],
        name="forward",
        compiler_params=PARAMS,
    )(*far(field, tz, wy))


def x_forward_kernel(s_ref, wx_ref, o_ref):
    high, low = split(s_ref[...])
    out = dot(wx_ref[...], high)
    o_ref[...] = out[: 2 * MX] + out[2 * MX :] + dot(wx_ref[: 2 * MX], low)


def x_forward(sent, wx):
    return pl.pallas_call(
        x_forward_kernel,
        in_specs=[VMEM] * 2,
        out_specs=VMEM,
        out_shape=pltpu.VMEM((2 * MX, LC * K8), F32),
        name="x_forward",
        compiler_params=PARAMS,
    )(*near(sent, wx))


def mix_kernel(x_ref, w_ref, vx_ref, o_ref):
    lanes = LC * K8
    within = lax.broadcasted_iota(jnp.int32, (MX, lanes), 1) % K8
    real_g = jnp.zeros((MX, lanes), F32)
    imag_g = jnp.zeros((MX, lanes), F32)
    for i in range(C):
        at = within + (i % LC) * K8
        real = jnp.take_along_axis(x_ref[i // LC, :MX], at, axis=1)
        imag = jnp.take_along_axis(x_ref[i // LC, MX:], at, axis=1)
        w_re, w_im = w_ref[0, i], w_ref[1, i]
        real_g += w_re * real - w_im * imag
        imag_g += w_re * imag + w_im * real
    high, low = split(jnp.concatenate([real_g, imag_g], 0))
    o_ref[...] = dot(vx_ref[...], jnp.concatenate([high, high, low], 0))


def mix(both, weights, vx):
    return pl.pallas_call(
        mix_kernel,
        in_specs=[VMEM] * 3,
        out_specs=VMEM,
        out_shape=pltpu.VMEM((2 * NX, LC * K8), F32),
        name="mix",
        compiler_params=PARAMS,
    )(*near(both, weights, vx))


BYPASS_ROWS = 16


def bypass_kernel(core_ref, bias_ref, w_ref, f_ref, g_ref, vy_in, vz_in, o_ref, field_ref, vy_ref, vz_ref, w2_ref):
    rows = LC * BYPASS_ROWS
    step = pl.program_id(0)

    @pl.when(step == 0)
    def _():
        row_of = lax.broadcasted_iota(jnp.int32, (rows, LC), 0) // BYPASS_ROWS
        left = (row_of == lax.broadcasted_iota(jnp.int32, (rows, LC), 1)).astype(BF16)
        same = (
            lax.broadcasted_iota(jnp.int32, (rows, rows), 0) % BYPASS_ROWS
            == lax.broadcasted_iota(jnp.int32, (rows, rows), 1) % BYPASS_ROWS
        )
        col_of = lax.broadcasted_iota(jnp.int32, (C, rows), 1) // BYPASS_ROWS
        channel = lax.broadcasted_iota(jnp.int32, (C, rows), 0)
        core = core_ref[0]
        for n, part in enumerate(split(0.5 * w_ref[...])):
            tall = dot(left, part).astype(BF16)
            for k in range(2):
                first = LC * (core if k == 0 else 1 - core)
                pick = (channel == col_of + first).astype(BF16)
                w2_ref[k, n] = jnp.where(same, dot(tall, pick), 0.0).astype(BF16)
        vy_ref[...] = vy_in[...]
        vz_ref[...] = vz_in[...]

    at = pl.multiple_of(step * BYPASS_ROWS, BYPASS_ROWS)
    total = None
    for k, ref in enumerate((f_ref, g_ref)):
        block = ref[...].reshape(rows, NZ)
        term = dot(w2_ref[k, 0], block) + dot(w2_ref[k, 1], block)
        total = term if total is None else total + term
    field_ref[:, pl.ds(at, BYPASS_ROWS), :] = f_ref[...]
    for o in range(LC):
        o_ref[o, pl.ds(at, BYPASS_ROWS), :] = total[o * BYPASS_ROWS : (o + 1) * BYPASS_ROWS] + 0.5 * bias_ref[0, o]


def bypass_of(core, bias, weights, own, other, vy, vz):
    rows = LC * BYPASS_ROWS
    smem = pl.BlockSpec(memory_space=pltpu.SMEM)
    whole = pl.BlockSpec(weights.shape, lambda s: (0, 0))
    block = pl.BlockSpec((LC, BYPASS_ROWS, NZ), lambda s: (0, s, 0))
    return pl.pallas_call(
        bypass_kernel,
        grid=(NY // BYPASS_ROWS,),
        in_specs=[smem, smem, whole, block, block]
        + [pl.BlockSpec(v.shape, lambda s, n=v.ndim: (0,) * n) for v in (vy, vz)],
        out_specs=[VMEM] * 4,
        out_shape=[pltpu.VMEM((LC, NY, NZ), F32), pltpu.VMEM((LC, NY, NZ), BF16), pltpu.VMEM(vy.shape, BF16), pltpu.VMEM(vz.shape, BF16)],
        scratch_shapes=[pltpu.VMEM((2, 2, rows, rows), BF16)],
        name="bypass",
        compiler_params=PARAMS,
    )(core, bias, *far(weights, own, other, vy, vz))


def stage_kernel(w_ref, wx_in, vx_in, o_ref, wx_ref, vx_ref):
    wx_ref[...] = wx_in[...]
    vx_ref[...] = vx_in[...]
    for part in range(2):
        for j in range(MX):
            o_ref[part, :, j, :] = w_ref[part, j].astype(F32).T


def stage(weights, wx, vx):
    return pl.pallas_call(
        stage_kernel,
        out_specs=[VMEM] * 3,
        out_shape=[
            pltpu.VMEM((2, C, MX, LC * K8), F32),
            pltpu.VMEM(wx.shape, BF16),
            pltpu.VMEM(vx.shape, BF16),
        ],
        name="stage",
        compiler_params=PARAMS,
    )(*far(weights, wx, vx))


GELU = float(np.sqrt(2.0 / np.pi))
TOGETHER = 2


def inverse_kernel(h_ref, vy_ref, vz_ref, b_ref, f_ref, o_hbm, a_ref, out_ref, sems):
    sides = []
    for b in range(KB):
        sides.append(jnp.concatenate([h_ref[rows_of(b, n, part), :] for part in range(2) for n in range(PX)], 0).T)
    high, low = split(jnp.concatenate(sides, 0))
    a_ref[...] = dot(high, vy_ref[0]) + dot(low, vy_ref[0]) + dot(high, vy_ref[1])

    copies = []
    for o in range(LC):
        parts = [
            a_ref[b * LC * K8 + o * K8 : b * LC * K8 + (o + 1) * K8, part * NY : (part + 1) * NY]
            for part in range(2)
            for b in range(KB)
        ]
        high, low = split(jnp.concatenate(parts, 0))
        half = dot(jnp.concatenate([high, low, high], 0).T, vz_ref[...]) + b_ref[o]
        bend = jnp.tanh(half * (2.0 * GELU + (8.0 * 0.044715 * GELU) * (half * half)))
        out_ref[o] = (f_ref[o].astype(F32) + half) + half * bend
        if (o + 1) % TOGETHER == 0:
            rows = pl.ds(o + 1 - TOGETHER, TOGETHER)
            copies.append(pltpu.make_async_copy(out_ref.at[rows], o_hbm.at[rows], sems.at[o // TOGETHER]))
            copies[-1].start()
    for copy in copies:
        copy.wait()


def inverse(sent, vy, vz, pre, field):
    return pl.pallas_call(
        inverse_kernel,
        in_specs=[VMEM] * 5,
        out_specs=pl.BlockSpec(memory_space=pl.ANY),
        out_shape=jax.ShapeDtypeStruct((LC, NY, NZ), F32),
        scratch_shapes=[
            pltpu.VMEM((KB * LC * K8, 2 * NY), F32),
            pltpu.VMEM((LC, NY, NZ), F32),
            pltpu.SemaphoreType.DMA((LC // TOGETHER,)),
        ],
        name="inverse",
        compiler_params=PARAMS,
    )(*near(sent, vy, vz, pre, field))


def exchange(value):
    sent = value.astype(F16).reshape(NX, 2, LC * K8)
    sent = lax.all_to_all(sent, "pen", 0, 0, axis_index_groups=[ORDER], tiled=True)
    return sent.reshape(2 * NX, LC * K8).astype(F32)


def local(features, spectral_weights, bypass_weights, bypass_bias):
    tz, wy, wx, vx, vy, vz = constants()
    field = features[0]
    other = lax.ppermute(field, "ch", [(0, 1), (1, 0)])

    modes = exchange(forward(field, tz, wy))

    core = lax.axis_index("ch").astype(jnp.int32)[None]
    pre, near_field, vy, vz = bypass_of(core, bypass_bias, bypass_weights[0].T, field, other, vy, vz)

    weights = spectral_weights[0].transpose(0, 1, 3, 4, 2).reshape(2, MX, LC * K8, C)
    weights, wx, vx = stage(weights, wx, vx)
    both = lax.all_gather(x_forward(modes, wx), "ch")
    back = exchange(mix(both, weights, vx))
    return inverse(back, vy, vz, pre, near_field)[None]


def solution(mesh):
    return jax.shard_map(
        local,
        mesh=mesh,
        in_specs=(
            P(("grp", "pen"), "ch", None, None),
            P(None, None, None, None, "ch", "pen"),
            P(None, None, "ch"),
            P(None, "ch"),
        ),
        out_specs=P(("grp", "pen"), "ch", None, None),
        check_vma=False,
    )
```
